256 devices in a mesh: tm: 32 (over z, y), grid: 8 (over x, core).
Axes of the slice: x: 4, y: 4, z: 8, core: 2. Of those that a mesh axis runs over, the one named last changes fastest.
Arguments:
- departure: float32 [64, 128, 3, 1024], P('tm', 'grid'), may hold values from -6 to 6
- obs_weight: float32 [64, 128], P('tm', 'grid'), may hold values from 0.2 to 2
- obs_block: int32 [64, 128], P('tm', 'grid'), may hold values from 0 to 7
- coarse_decay: float32 [3, 64, 1024], P(None, 'grid'), may hold values from 0.95 to 1
Outputs:
- adjoint: float32 [64, 3, 64, 1024], P('tm', None, 'grid')
- misfit: float32 [], replicated
- changes: float32 [3], replicated
The draws below stay inside these ranges and needn't reach their ends.
Inputs may be any that keep to these rules, and one draw needn't show every extreme that they name: `obs_block`: several observations may name the same block.
All inputs are finite; a program needn't handle non-finite values.
Results may differ from the reference program's by a relative error of at most 0.0003.
Values sent between devices are 32-bit elements; how exact they have to be, the bound alone decides.
No kernel may reach another device: no remote copies, remote signals or barrier semaphores. Data moves between devices by JAX's collectives and lax.ppermute only.
A program may use at most 64 MiB of HBM per device.

```python
import math
import jax
import jax.numpy as jnp
from jax import lax

ROWS_DEV = 8
NLON = 1024
OBS_DEV = 16
STEPS = 4
ITERS = 3
TILE_ROWS = 8
TILE_COLS = 128
SUBWINDOWS = 64
NLAT = 64
OBS = 128
TILE = 1024
BLOCKS_DEV = 8
N_GRID = 8


def plant(drawn, stream_key, low, largest):
    shape = drawn.shape
    index_at = [jax.random.randint(jax.random.fold_in(stream_key, axis), (), 0, shape[axis]) for axis in range(len(shape))]
    drawn = drawn.at[tuple(index_at)].set(low)
    longest = shape.index(max(shape))
    index_at[longest] = (index_at[longest] + 1) % shape[longest]
    return drawn.at[tuple(index_at)].set(largest)


def steps_of(stream_key, dims, split, smallest, largest):
    def one(axis_at, blocks):
        steps = jax.random.uniform(jax.random.fold_in(jax.random.fold_in(stream_key, 6), axis_at), (blocks,), jnp.float32, smallest / len(split), largest / len(split))
        return jnp.repeat(jnp.exp(steps), dims[axis_at] // blocks).reshape((-1,) + (1,) * (len(dims) - axis_at - 1))

    loudness = one(*split[0])
    for cut in split[1:]:
        loudness = loudness * one(*cut)
    return loudness


def noise(rng, dims, scale, reach, cuts=(), kind=jnp.bfloat16):
    entries = jax.random.normal(rng, dims, jnp.float32) * scale
    if len(cuts) > 0:
        entries = steps_of(rng, dims, cuts, -0.22, 0.18) * entries
    return jnp.clip(entries, min=-reach, max=reach).astype(kind)


def setup_inputs(seed: int = 0) -> dict:
    key_of = jax.random.split(jax.random.key(seed), 5)
    return {
        "departure": noise(key_of[0], (SUBWINDOWS, OBS, 3, TILE), 1.0, 6.0, ((0, 32), (1, 8)), jnp.float32),
        "obs_weight": jnp.clip(jnp.exp(math.log(2.0) - 2.3025851 * jax.random.uniform(key_of[1], (SUBWINDOWS, OBS), jnp.float32) ** steps_of(key_of[1], (SUBWINDOWS, OBS), ((0, 32), (1, 8)), -0.2, 0.2)), 0.2, 2.0),
        "obs_block": plant(jax.random.randint(key_of[2], (SUBWINDOWS, OBS), 0, BLOCKS_DEV), jax.random.fold_in(key_of[2], 1), 0, BLOCKS_DEV - 1).astype(jnp.int32),
        "coarse_decay": jnp.clip(0.95 + 0.050000012 * jax.random.uniform(key_of[3], (3, NLAT, NLON), jnp.float32) ** steps_of(key_of[3], (3, NLAT, NLON), ((1, 8),), -0.2, 0.2), 0.95, 1.0),
    }


wave_coef = 0.6
diffusion = 0.05
coriolis = 0.1
epsilon = 1e-6


def along_lon(values):
    return 0.5 * (jnp.roll(values, -1, -1) - jnp.roll(values, 1, -1))


def pad_rows(values):
    return jnp.pad(values, ((0, 0), (1, 1), (0, 0)))


def along_lat(values):
    padded = pad_rows(values)
    return 0.5 * (padded[:, 2:] - padded[:, :-2])


def laplace(values):
    padded = pad_rows(values)
    return padded[:, 2:] + padded[:, :-2] + jnp.roll(values, -1, -1) + jnp.roll(values, 1, -1) - 4.0 * values


def sweep_once(fields, inside):
    height, zonal, merid = fields[:, 0], fields[:, 1], fields[:, 2]
    weight = inside[None, :, None]
    height_new = (height + wave_coef * (along_lon(zonal) + along_lat(merid)) + diffusion * laplace(height)) * weight
    zonal_new = (zonal + wave_coef * along_lon(height_new) + coriolis * merid + diffusion * laplace(zonal)) * weight
    merid_new = (merid + wave_coef * along_lat(height_new) - coriolis * zonal + diffusion * laplace(merid)) * weight
    return jnp.stack([height_new, zonal_new, merid_new], axis=1)


def spread_tiles(scaled, blocks, row_count, lon_count):
    tile_rows_n = row_count // TILE_ROWS
    tile_cols_n = lon_count // TILE_COLS
    choose = (blocks[..., None] == jnp.arange(tile_rows_n * tile_cols_n, dtype=jnp.int32)).astype(jnp.float32)
    tiles = jnp.einsum("sob,soct->sbct", choose, scaled, precision=lax.Precision.HIGHEST)
    leading = scaled.shape[0]
    tiles = tiles.reshape(leading, tile_rows_n, tile_cols_n, 3, TILE_ROWS, TILE_COLS).transpose(0, 3, 1, 4, 2, 5)
    return tiles.reshape(leading, 3, row_count, lon_count)


def reference(departure, obs_weight, obs_block, coarse_decay):
    count = SUBWINDOWS
    emphasis = 1.0 + 2.0 * jnp.arange(count, dtype=jnp.float32) / (count - 1)
    misfit = 0.5 * jnp.sum(emphasis[:, None] * obs_weight * jnp.sum(departure * departure, axis=(2, 3)))
    scaled = departure * (emphasis[:, None] * obs_weight)[:, :, None, None]
    scaled = scaled.reshape(count * N_GRID, OBS_DEV, 3, TILE)
    blocks = obs_block.reshape(count * N_GRID, OBS_DEV)
    forcing = spread_tiles(scaled, blocks, ROWS_DEV, NLON)
    forcing = forcing.reshape(count, N_GRID, 3, ROWS_DEV, NLON).transpose(0, 2, 1, 3, 4).reshape(count, 3, NLAT, NLON)
    inside = jnp.ones((NLAT,), jnp.float32)

    def fine(fields):
        for repeat in range(STEPS):
            fields = sweep_once(fields, inside)
        return fields

    def backward(correction):
        def advance(carry, term):
            value = coarse_decay * carry + term
            return value, value
        start = jnp.zeros((3, NLAT, NLON), jnp.float32)
        return lax.scan(advance, start, correction, reverse=True)[1]

    adjoint = backward(forcing)
    changes = []
    for iteration in range(ITERS):
        above = jnp.concatenate([adjoint[1:], jnp.zeros_like(adjoint[:1])], axis=0)
        correction = fine(above) - coarse_decay * above + forcing
        renewed = backward(correction)
        weights = emphasis[:, None, None, None]
        change_sum = jnp.sum(weights * (renewed - adjoint) ** 2)
        size_sum = jnp.sum(weights * renewed ** 2)
        changes.append(change_sum / (size_sum + epsilon))
        adjoint = renewed
    return adjoint, misfit, jnp.stack(changes)
```

```python
import functools

import jax
import jax.numpy as jnp
from jax import lax
from jax.experimental import pallas as pl
from jax.experimental.pallas import tpu as pltpu
from jax.sharding import Mesh
from jax.sharding import PartitionSpec as P

STEPS = 4
ITERS = 3
NZ, NY, NX = 8, 4, 4
CHIPS = NZ * NY * NX
LONS = 8
FIELDS = 3
TM = ("z", "y")
GRID = ("x", "c")
ZYX = ("z", "y", "x")

wave_coef = 0.6
diffusion = 0.05
coriolis = 0.1
epsilon = 1e-06


def chip_of(tile):
    z, place = divmod(tile, NY * NX)
    if z % 2:
        place = NY * NX - 1 - place
    y, x = divmod(place, NX)
    if y % 2:
        x = NX - 1 - x
    return (z * NY + y) * NX + x


def swap_pairs(first):
    pairs = []
    for tile in range(first, CHIPS, 2):
        a, b = chip_of(tile), chip_of((tile + 1) % CHIPS)
        pairs += [(a, b), (b, a)]
    return pairs


SIBLING = [(0, 1), (1, 0)]


def shape(*dims):
    return jax.ShapeDtypeStruct(dims, jnp.float32)


def call(kernel, outs, scalars, *operands, scratch=()):
    vmem = pl.BlockSpec(memory_space=pltpu.VMEM)
    smem = pl.BlockSpec(memory_space=pltpu.SMEM)
    return pl.pallas_call(
        kernel,
        out_shape=outs,
        in_specs=[smem] * len(scalars) + [vmem] * len(operands),
        out_specs=jax.tree.map(lambda _: vmem, outs),
        scratch_shapes=list(scratch),
    )(*scalars, *operands)


def iota(dim):
    return lax.broadcasted_iota(jnp.int32, (8, 128), dim)


def pack_kernel(odd_ref, tiles_ref, decay_ref, out_ref, rows_ref):
    odd = odd_ref[0] == 1
    for j in range(2):
        for f in range(FIELDS):
            for r in range(8):
                rows_ref[pl.ds(24 * j + 8 * f + r, 8, stride=64), :] = tiles_ref[
                    j, f, :, 128 * r : 128 * r + 128
                ]
    for b in range(8):
        span = slice(128 * b, 128 * b + 128)
        rows_ref[64 * b + 48 : 64 * b + 56, :] = jnp.where(
            odd, decay_ref[2, :, span], decay_ref[0, :, span]
        )
        rows_ref[64 * b + 56 : 64 * b + 64, :] = decay_ref[1, :, span]
    for b in range(8):
        block = rows_ref[64 * b : 64 * b + 64, :]
        both = jnp.concatenate([block, pltpu.roll(block, 124, 1)], axis=0)
        turned = both.T
        for i in range(16):
            to = 4 * chip_of(16 * b + i)
            out_ref[to : to + 4, :] = turned[8 * i : 8 * i + 4, :]


def later(value, groups):
    return pltpu.roll(value, 128 - 8 * groups, value.ndim - 1)


def scan_pairs(u, square, pair):
    factor = square
    for groups in (1, 2, 4, 8):
        u = u + jnp.where(pair < 16 - groups, factor, 0.0) * later(u, groups)
        factor = factor * factor
    return u


def chain_here(c0, c1, decay, pair, first_ref, second_ref, carry_ref, at):
    square = decay * decay
    value = scan_pairs(c0 + decay * c1, square, pair)
    first_ref[at] = value
    second_ref[at] = c1 + decay * jnp.where(pair < 15, later(value, 1), 0.0)
    spread = jnp.where(pair < 1, value, 0.0)
    for groups in (1, 2, 4, 8):
        spread = spread + pltpu.roll(spread, 8 * groups, spread.ndim - 1)
    carry_ref[at] = spread


def open_kernel(
    core_ref, mine_ref, other_ref, first_ref, second_ref, carry_ref, decay_ref, power_ref, turn_ref
):
    low = core_ref[0] == 0
    lane = iota(1)
    pair = lane // 8
    even = (pair & 1) == 0
    for s in range(4):
        below = mine_ref[pl.ds(s, 64, stride=4), :]
        above = mine_ref[pl.ds(256 + s, 64, stride=4), :]
        kept = jnp.where(low, below, above)
        got = other_ref[pl.ds(s, 64, stride=4), :]
        turn_ref[pl.ds(0, 64, stride=2), :] = jnp.where(low, kept, got)
        turn_ref[pl.ds(1, 64, stride=2), :] = jnp.where(low, got, kept)
        turned = turn_ref[...].T
        for half in range(2):
            at = 64 * half
            col = s + 4 * half
            mixed = turned[at + 48 : at + 56, :]
            decays = (
                jnp.where(even, mixed, pltpu.roll(mixed, 8, 1)),
                turned[at + 56 : at + 64, :],
                jnp.where(even, pltpu.roll(mixed, 120, 1), mixed),
            )
            for f in range(FIELDS):
                decay = decays[f]
                c0 = turned[at + 8 * f : at + 8 * f + 8, :]
                c1 = turned[at + 24 + 8 * f : at + 32 + 8 * f, :]
                decay_ref[f, col] = decay
                chain_here(c0, c1, decay, pair, first_ref, second_ref, carry_ref, (f, col))
                power = decay * decay
                for groups in (1, 2, 4, 8):
                    power = power * jnp.where(pair < 16 - groups, later(power, groups), 1.0)
                power_ref[0, f, col] = power
                power_ref[1, f, col] = decay * jnp.where(pair < 15, later(power, 1), 1.0)


def close_kernel(core_ref, first_ref, second_ref, carry_ref, power_ref, zero_ref, above_ref):
    low = core_ref[0] == 0
    pair = iota(1) // 8
    for f in range(FIELDS):
        for col in range(LONS):
            carry = jnp.where(low, carry_ref[f, col], 0.0)
            value = first_ref[f, col] + power_ref[0, f, col] * carry
            zero_ref[f, col] = value
            above_ref[0, f, col] = second_ref[f, col] + power_ref[1, f, col] * carry
            above_ref[1, f, col] = jnp.where(pair < 15, later(value, 1), carry)


def fine_kernel(
    odd_ref, own_ref, even_ref, odd_side_ref, decay_ref, first_ref, second_ref, carry_ref, state_ref
):
    odd = odd_ref[0] == 1
    row = iota(0)[None]
    lane = iota(1)[None]
    band = lane % 8
    pair = lane // 8
    at_top = row == 0
    at_end = row == 7
    not_first = band > 0
    not_last = band < 7

    def next_row(v):
        inner = pltpu.roll(v, 7, 1)
        edge = jnp.where(not_last, pltpu.roll(inner, 127, 2), 0.0)
        return jnp.where(at_end, edge, inner)

    def last_row(v):
        inner = pltpu.roll(v, 1, 1)
        edge = jnp.where(not_first, pltpu.roll(inner, 1, 2), 0.0)
        return jnp.where(at_top, edge, inner)

    corrections = []
    for j in range(2):
        for f in range(FIELDS):
            one, two = even_ref[j, f], odd_side_ref[j, f]
            state_ref[f, 0:8] = jnp.where(odd, one, two)
            state_ref[f, 8:16] = own_ref[j, f]
            state_ref[f, 16:24] = jnp.where(odd, two, one)
        p, q, r = state_ref[0], state_ref[1], state_ref[2]
        keep = 1.0 - 4.0 * diffusion
        wave = 0.5 * wave_coef
        for step in range(STEPS):
            n = p.shape[0]
            inside = slice(1, n - 1)
            pc, rc = p[inside], r[inside]
            p1 = (
                keep * pc
                + diffusion * (p[: n - 2] + p[2:])
                + wave * (q[2:] - q[: n - 2])
                + next_row(diffusion * pc + wave * rc)
                + last_row(diffusion * pc - wave * rc)
            )
            m = n - 2
            q2, r2, p2 = q[inside], rc, p1
            qc, rcc, pcc = q2[1 : m - 1], r2[1 : m - 1], p2[1 : m - 1]
            scaled = diffusion * qc
            q1 = (
                keep * qc
                + diffusion * (q2[: m - 2] + q2[2:])
                + wave * (p2[2:] - p2[: m - 2])
                + coriolis * rcc
                + next_row(scaled)
                + last_row(scaled)
            )
            r1 = (
                keep * rcc
                + diffusion * (r2[: m - 2] + r2[2:])
                - coriolis * qc
                + next_row(diffusion * rcc + wave * pcc)
                + last_row(diffusion * rcc - wave * pcc)
            )
            p, q, r = pcc, q1, r1
        corrections.append([v - decay_ref[f] * own_ref[j, f] for f, v in enumerate((p, q, r))])
    for f in range(FIELDS):
        chain_here(
            corrections[0][f], corrections[1][f], decay_ref[f], pair, first_ref, second_ref, carry_ref, f
        )


def finish_kernel(core_ref, *refs):
    zeros = refs[0:3]
    aboves = refs[3:6]
    first_ref, second_ref, carry_ref, power_ref, misfit_ref, ones_ref = refs[6:12]
    mine_ref, other_ref, turn_ref = refs[12:]
    low = core_ref[0] == 0
    pair = iota(1) // 8
    subwindow = (2 * (pair + jnp.where(low, 0, 16))).astype(jnp.float32)
    emphasis = [1.0 + 2.0 * (subwindow + j) / 63.0 for j in range(2)]
    sums = [jnp.zeros((8, 128), jnp.float32) for _ in range(2 * ITERS)]
    result = {}
    for f in range(FIELDS):
        for col in range(LONS):
            carry = jnp.where(low, carry_ref[f, col], 0.0)
            last = (
                first_ref[f, col] + power_ref[0, f, col] * carry,
                second_ref[f, col] + power_ref[1, f, col] * carry,
            )
            for j in range(2):
                so_far = zeros[0][f, col] if j == 0 else aboves[0][0, f, col]
                for n in range(ITERS):
                    if n == ITERS - 1:
                        change = last[j]
                    else:
                        change = zeros[n + 1][f, col] if j == 0 else aboves[n + 1][0, f, col]
                    so_far = so_far + change
                    sums[n] = sums[n] + emphasis[j] * (change * change)
                    sums[ITERS + n] = sums[ITERS + n] + emphasis[j] * (so_far * so_far)
                result[j, f, col] = so_far
    parts = jnp.concatenate(sums + [misfit_ref[...], jnp.zeros((8, 128), jnp.float32)], axis=0)
    totals = jnp.dot(parts, ones_ref[...], precision=lax.Precision.HIGHEST)
    for s in range(4):
        for half in range(2):
            at = 64 * half
            for j in range(2):
                for f in range(FIELDS):
                    to = at + 24 * j + 8 * f
                    turn_ref[to : to + 8, :] = result[j, f, s + 4 * half]
            if s < 2:
                which = 4 * half + 2 * s
                turn_ref[at + 48 : at + 64, :] = totals[8 * which : 8 * which + 16, :]
        back = turn_ref[...].T
        turn_ref[...] = back
        evens = turn_ref[pl.ds(0, 64, stride=2), :]
        odds = turn_ref[pl.ds(1, 64, stride=2), :]
        mine_ref[pl.ds(s, 64, stride=4), :] = jnp.where(low, evens, odds)
        other_ref[pl.ds(s, 64, stride=4), :] = jnp.where(low, odds, evens)


def join_kernel(core_ref, mine_ref, got_ref, out_ref):
    low = core_ref[0] == 0
    lane = lax.broadcasted_iota(jnp.int32, (256, 128), 1)
    counted = (lane & 63) >= 48
    mine, got = mine_ref[...], got_ref[...]
    total = mine + got
    out_ref[0:256, :] = jnp.where(counted, total, jnp.where(low, mine, got))
    out_ref[256:512, :] = jnp.where(counted, total, jnp.where(low, got, mine))


def unpack_kernel(in_ref, out_ref, sums_ref, rows_ref):
    total = in_ref[0:8, :]
    for v in range(1, 64):
        total = total + in_ref[8 * v : 8 * v + 8, :]
    sums_ref[...] = total
    second = (lax.broadcasted_iota(jnp.int32, (128, 128), 0) & 7) >= 4
    for b in range(8):
        for i in range(16):
            at = 4 * chip_of(16 * b + i)
            piece = in_ref[at : at + 4, :]
            rows_ref[8 * i : 8 * i + 4, :] = piece
            rows_ref[8 * i + 4 : 8 * i + 8, :] = piece
        block = rows_ref[...]
        turned = jnp.where(second, pltpu.roll(block, 64, 1), block).T
        for j in range(2):
            for f in range(FIELDS):
                at = 24 * j + 8 * f
                out_ref[j, f, :, 128 * b : 128 * b + 128] = turned[at : at + 8, :]


def per_device(departure, obs_weight, obs_block, coarse_decay):
    z, y, x, core = (lax.axis_index(name) for name in ("z", "y", "x", "c"))
    core_arg = core.astype(jnp.int32).reshape(1)
    tile_odd = ((x + y + z) % 2).astype(jnp.int32).reshape(1)
    pair_odd = (y % 2).astype(jnp.int32).reshape(1)

    position = ((z * NY + y) * 2 + jnp.arange(2)).astype(jnp.float32)
    emphasis = 1.0 + 2.0 * position / 63.0
    strength = emphasis[:, None] * obs_weight
    misfit_part = 0.5 * jnp.sum(
        strength[:, :, None, None] * departure * departure, axis=(0, 1, 2)
    ).reshape(8, 128)
    choose = jnp.where(
        obs_block[:, :, None] == jnp.arange(8, dtype=jnp.int32), strength[:, :, None], 0.0
    )
    tiles = jnp.einsum("sob,soct->scbt", choose, departure, precision=lax.Precision.HIGHEST)

    sent = call(
        pack_kernel,
        shape(512, 128),
        (pair_odd,),
        tiles,
        coarse_decay,
        scratch=[pltpu.VMEM((512, 128), jnp.float32)],
    )
    got = lax.all_to_all(sent.reshape(CHIPS, 4, 128), ZYX, 0, 0).reshape(512, 128)
    away = lax.dynamic_slice_in_dim(got, 256 * (1 - core), 256)
    other = lax.ppermute(away, "c", SIBLING)

    field = shape(FIELDS, LONS, 8, 128)
    both = shape(2, FIELDS, LONS, 8, 128)
    square = pltpu.VMEM((128, 128), jnp.float32)
    first, second, carry, decay, power = call(
        open_kernel, (field, field, field, field, both), (core_arg,), got, other, scratch=[square]
    )
    zeros, aboves = [], []
    for _ in range(ITERS):
        carry = lax.ppermute(carry, "c", SIBLING)
        zero, above = call(
            close_kernel, (field, both), (core_arg,), first, second, carry, power
        )
        zeros.append(zero)
        aboves.append(above)
        side_even = lax.ppermute(above, ZYX, swap_pairs(0))
        side_odd = lax.ppermute(above, ZYX, swap_pairs(1))
        first, second, carry = call(
            fine_kernel,
            (field, field, field),
            (tile_odd,),
            above,
            side_even,
            side_odd,
            decay,
            scratch=[pltpu.VMEM((FIELDS, 24, 8, 128), jnp.float32)],
        )
    carry = lax.ppermute(carry, "c", SIBLING)
    mine, away = call(
        finish_kernel,
        (shape(256, 128), shape(256, 128)),
        (core_arg,),
        *zeros,
        *aboves,
        first,
        second,
        carry,
        power,
        misfit_part,
        jnp.ones((128, 128), jnp.float32),
        scratch=[square],
    )
    other = lax.ppermute(away, "c", SIBLING)
    back = call(join_kernel, shape(512, 128), (core_arg,), mine, other)
    home = lax.all_to_all(back.reshape(CHIPS, 4, 128), ZYX, 0, 0).reshape(512, 128)
    adjoint, sums = call(
        unpack_kernel,
        (shape(2, FIELDS, 8, 1024), shape(8, 128)),
        (),
        home,
        scratch=[square],
    )
    counted = jnp.sum(sums.reshape(2, 4, 2, 64)[:, :2, :, 48:].reshape(2, 2, 2, 2, 8), axis=(0, 4))
    totals = counted.transpose(1, 0, 2).reshape(8)
    changes = totals[:ITERS] / (totals[ITERS : 2 * ITERS] + epsilon)
    return adjoint, totals[2 * ITERS], changes


def solution(mesh):
    split = Mesh(mesh.devices.reshape(NZ, NY, NX, 2), ("z", "y", "x", "c"))
    return jax.shard_map(
        per_device,
        mesh=split,
        in_specs=(P(TM, GRID, None, None), P(TM, GRID), P(TM, GRID), P(None, GRID, None)),
        out_specs=(P(TM, None, GRID, None), P(), P()),
        check_vma=False,
    )
```

```python
import functools

import jax
import jax.numpy as jnp
from jax import lax
from jax.experimental import pallas as pl
from jax.experimental.pallas import tpu as pltpu
from jax.sharding import Mesh
from jax.sharding import PartitionSpec as P

STEPS = 4
ITERS = 3
NZ, NY, NX = 8, 4, 4
CHIPS = NZ * NY * NX
LONS = 8
FIELDS = 3
TM = ("z", "y")
GRID = ("x", "c")
ZYX = ("z", "y", "x")

wave_coef = 0.6
diffusion = 0.05
coriolis = 0.1
epsilon = 1e-06


def chip_of(tile):
    z, place = divmod(tile, NY * NX)
    if z % 2:
        place = NY * NX - 1 - place
    y, x = divmod(place, NX)
    if y % 2:
        x = NX - 1 - x
    return (z * NY + y) * NX + x


def swap_pairs(first):
    pairs = []
    for tile in range(first, CHIPS, 2):
        a, b = chip_of(tile), chip_of((tile + 1) % CHIPS)
        pairs += [(a, b), (b, a)]
    return pairs


SIBLING = [(0, 1), (1, 0)]


def shape(*dims):
    return pltpu.VMEM(dims, jnp.float32)


def near(value):
    return pltpu.with_memory_space_constraint(value, pltpu.VMEM)


def call(kernel, outs, scalars, *operands, scratch=()):
    vmem = pl.BlockSpec(memory_space=pltpu.VMEM)
    smem = pl.BlockSpec(memory_space=pltpu.SMEM)
    return pl.pallas_call(
        kernel,
        out_shape=outs,
        in_specs=[smem] * len(scalars) + [vmem] * len(operands),
        out_specs=jax.tree.map(lambda _: vmem, outs),
        scratch_shapes=list(scratch),
    )(*scalars, *map(near, operands))


def iota(dim):
    return lax.broadcasted_iota(jnp.int32, (8, 128), dim)


def pack_kernel(odd_ref, tiles_ref, decay_ref, out_ref, rows_ref):
    odd = odd_ref[0] == 1
    for j in range(2):
        for f in range(FIELDS):
            for r in range(8):
                rows_ref[pl.ds(24 * j + 8 * f + r, 8, stride=64), :] = tiles_ref[
                    j, f, :, 128 * r : 128 * r + 128
                ]
    for b in range(8):
        span = slice(128 * b, 128 * b + 128)
        rows_ref[64 * b + 48 : 64 * b + 56, :] = jnp.where(
            odd, decay_ref[2, :, span], decay_ref[0, :, span]
        )
        rows_ref[64 * b + 56 : 64 * b + 64, :] = decay_ref[1, :, span]
    for b in range(8):
        block = rows_ref[64 * b : 64 * b + 64, :]
        both = jnp.concatenate([block, pltpu.roll(block, 124, 1)], axis=0)
        turned = both.T
        for i in range(16):
            to = 4 * chip_of(16 * b + i)
            out_ref[to : to + 4, :] = turned[8 * i : 8 * i + 4, :]


def later(value, groups):
    return pltpu.roll(value, 128 - 8 * groups, value.ndim - 1)


def scan_pairs(u, square, pair):
    factor = square
    for groups in (1, 2, 4, 8):
        u = u + jnp.where(pair < 16 - groups, factor, 0.0) * later(u, groups)
        factor = factor * factor
    return u


def chain_here(c0, c1, decay, pair, first_ref, second_ref, carry_ref, at):
    square = decay * decay
    value = scan_pairs(c0 + decay * c1, square, pair)
    first_ref[at] = value
    second_ref[at] = c1 + decay * jnp.where(pair < 15, later(value, 1), 0.0)
    spread = jnp.where(pair < 1, value, 0.0)
    for groups in (1, 2, 4, 8):
        spread = spread + pltpu.roll(spread, 8 * groups, spread.ndim - 1)
    carry_ref[at] = spread


def open_kernel(
    core_ref, mine_ref, other_ref, first_ref, second_ref, carry_ref, decay_ref, power_ref, turn_ref
):
    low = core_ref[0] == 0
    lane = iota(1)
    pair = lane // 8
    even = (pair & 1) == 0
    for s in range(4):
        kept, got = (
            jnp.where(low, ref[pl.ds(s, 64, stride=4), :], ref[pl.ds(256 + s, 64, stride=4), :])
            for ref in (mine_ref, other_ref)
        )
        turn_ref[pl.ds(0, 64, stride=2), :] = jnp.where(low, kept, got)
        turn_ref[pl.ds(1, 64, stride=2), :] = jnp.where(low, got, kept)
        turned = turn_ref[...].T
        for half in range(2):
            at = 64 * half
            col = s + 4 * half
            mixed = turned[at + 48 : at + 56, :]
            decays = (
                jnp.where(even, mixed, pltpu.roll(mixed, 8, 1)),
                turned[at + 56 : at + 64, :],
                jnp.where(even, pltpu.roll(mixed, 120, 1), mixed),
            )
            for f in range(FIELDS):
                decay = decays[f]
                c0 = turned[at + 8 * f : at + 8 * f + 8, :]
                c1 = turned[at + 24 + 8 * f : at + 32 + 8 * f, :]
                decay_ref[f, col] = decay
                chain_here(c0, c1, decay, pair, first_ref, second_ref, carry_ref, (f, col))
                power = decay * decay
                for groups in (1, 2, 4, 8):
                    power = power * jnp.where(pair < 16 - groups, later(power, groups), 1.0)
                power_ref[0, f, col] = power
                power_ref[1, f, col] = decay * jnp.where(pair < 15, later(power, 1), 1.0)


def close_kernel(core_ref, first_ref, second_ref, carry_ref, power_ref, zero_ref, above_ref):
    low = core_ref[0] == 0
    pair = iota(1) // 8
    for f in range(FIELDS):
        for col in range(LONS):
            carry = jnp.where(low, carry_ref[f, col], 0.0)
            value = first_ref[f, col] + power_ref[0, f, col] * carry
            zero_ref[f, col] = value
            above_ref[0, f, col] = second_ref[f, col] + power_ref[1, f, col] * carry
            above_ref[1, f, col] = jnp.where(pair < 15, later(value, 1), carry)


def fine_kernel(
    odd_ref, own_ref, even_ref, odd_side_ref, decay_ref, first_ref, second_ref, carry_ref, state_ref
):
    odd = odd_ref[0] == 1
    row = iota(0)[None]
    lane = iota(1)[None]
    band = lane % 8
    pair = lane // 8
    at_top = row == 0
    at_end = row == 7
    not_first = band > 0
    not_last = band < 7

    def next_row(v):
        inner = pltpu.roll(v, 7, 1)
        edge = jnp.where(not_last, pltpu.roll(inner, 127, 2), 0.0)
        return jnp.where(at_end, edge, inner)

    def last_row(v):
        inner = pltpu.roll(v, 1, 1)
        edge = jnp.where(not_first, pltpu.roll(inner, 1, 2), 0.0)
        return jnp.where(at_top, edge, inner)

    corrections = []
    for j in range(2):
        for f in range(FIELDS):
            one, two = even_ref[j, f], odd_side_ref[j, f]
            state_ref[f, 0:8] = jnp.where(odd, one, two)
            state_ref[f, 8:16] = own_ref[j, f]
            state_ref[f, 16:24] = jnp.where(odd, two, one)
        p, q, r = state_ref[0], state_ref[1], state_ref[2]
        keep = 1.0 - 4.0 * diffusion
        wave = 0.5 * wave_coef
        for step in range(STEPS):
            n = p.shape[0]
            inside = slice(1, n - 1)
            pc, rc = p[inside], r[inside]
            p1 = (
                keep * pc
                + diffusion * (p[: n - 2] + p[2:])
                + wave * (q[2:] - q[: n - 2])
                + next_row(diffusion * pc + wave * rc)
                + last_row(diffusion * pc - wave * rc)
            )
            m = n - 2
            q2, r2, p2 = q[inside], rc, p1
            qc, rcc, pcc = q2[1 : m - 1], r2[1 : m - 1], p2[1 : m - 1]
            scaled = diffusion * qc
            q1 = (
                keep * qc
                + diffusion * (q2[: m - 2] + q2[2:])
                + wave * (p2[2:] - p2[: m - 2])
                + coriolis * rcc
                + next_row(scaled)
                + last_row(scaled)
            )
            r1 = (
                keep * rcc
                + diffusion * (r2[: m - 2] + r2[2:])
                - coriolis * qc
                + next_row(diffusion * rcc + wave * pcc)
                + last_row(diffusion * rcc - wave * pcc)
            )
            p, q, r = pcc, q1, r1
        corrections.append([v - decay_ref[f] * own_ref[j, f] for f, v in enumerate((p, q, r))])
    for f in range(FIELDS):
        chain_here(
            corrections[0][f], corrections[1][f], decay_ref[f], pair, first_ref, second_ref, carry_ref, f
        )


def finish_kernel(core_ref, *refs):
    zeros = refs[0:3]
    aboves = refs[3:6]
    first_ref, second_ref, carry_ref, power_ref, misfit_ref = refs[6:11]
    mine_ref, other_ref, turn_ref, back_ref = refs[11:]
    low = core_ref[0] == 0
    pair = iota(1) // 8
    subwindow = (2 * (pair + jnp.where(low, 0, 16))).astype(jnp.float32)
    emphasis = [1.0 + 2.0 * (subwindow + j) / 63.0 for j in range(2)]
    sums = [jnp.zeros((8, 128), jnp.float32) for _ in range(2 * ITERS)]
    result = {}
    for f in range(FIELDS):
        for col in range(LONS):
            carry = jnp.where(low, carry_ref[f, col], 0.0)
            last = (
                first_ref[f, col] + power_ref[0, f, col] * carry,
                second_ref[f, col] + power_ref[1, f, col] * carry,
            )
            for j in range(2):
                so_far = zeros[0][f, col] if j == 0 else aboves[0][0, f, col]
                for n in range(ITERS):
                    if n == ITERS - 1:
                        change = last[j]
                    else:
                        change = zeros[n + 1][f, col] if j == 0 else aboves[n + 1][0, f, col]
                    so_far = so_far + change
                    sums[n] = sums[n] + emphasis[j] * (change * change)
                    sums[ITERS + n] = sums[ITERS + n] + emphasis[j] * (so_far * so_far)
                result[j, f, col] = so_far
    row = iota(0)
    parts = jnp.zeros((8, 128), jnp.float32)
    for at, part in enumerate(sums[:ITERS] + [misfit_ref[...]] + sums[ITERS:]):
        parts = jnp.where(row == at, jnp.sum(part, axis=0, keepdims=True), parts)
    ones = jnp.ones((128, 128), jnp.float32)
    totals = jnp.dot(parts, ones, precision=lax.Precision.HIGHEST)
    turn_ref[48:56, :] = totals
    for s in range(4):
        for half in range(2):
            at = 64 * half
            for j in range(2):
                for f in range(FIELDS):
                    to = at + 24 * j + 8 * f
                    turn_ref[to : to + 8, :] = result[j, f, s + 4 * half]
        back_ref[...] = turn_ref[...].T
        evens = back_ref[pl.ds(0, 64, stride=2), :]
        odds = back_ref[pl.ds(1, 64, stride=2), :]
        mine_ref[pl.ds(s, 64, stride=4), :] = jnp.where(low, evens, odds)
        other_ref[pl.ds(s, 64, stride=4), :] = jnp.where(low, odds, evens)


def join_kernel(core_ref, mine_ref, got_ref, out_ref):
    low = core_ref[0] == 0
    lane = lax.broadcasted_iota(jnp.int32, (256, 128), 1)
    counted = (lane & 120) == 48
    mine, got = mine_ref[...], got_ref[...]
    total = mine + got
    out_ref[0:256, :] = jnp.where(counted, total, jnp.where(low, mine, got))
    out_ref[256:512, :] = jnp.where(counted, total, jnp.where(low, got, mine))


def unpack_kernel(in_ref, out_ref, misfit_ref, changes_ref, rows_ref):
    sums = [in_ref[8 * v : 8 * v + 8, :] for v in range(64)]
    while len(sums) > 1:
        sums = [a + b for a, b in zip(sums[::2], sums[1::2])]
    total = pltpu.roll(sums[0] + pltpu.roll(sums[0], 4, 0), 80, 1)
    misfit_ref[...] = total[0:1, 3:4]
    changes_ref[...] = (total / (pltpu.roll(total, 124, 1) + epsilon))[0:1, 0:ITERS]
    second = (lax.broadcasted_iota(jnp.int32, (128, 128), 0) & 7) >= 4
    for b in range(8):
        for i in range(16):
            at = 4 * chip_of(16 * b + i)
            piece = in_ref[at : at + 4, :]
            rows_ref[8 * i : 8 * i + 4, :] = piece
            rows_ref[8 * i + 4 : 8 * i + 8, :] = piece
        block = rows_ref[...]
        turned = jnp.where(second, pltpu.roll(block, 64, 1), block).T
        for j in range(2):
            for f in range(FIELDS):
                at = 24 * j + 8 * f
                out_ref[j, f, :, 128 * b : 128 * b + 128] = turned[at : at + 8, :]


def per_device(departure, obs_weight, obs_block, coarse_decay):
    z, y, x, core = (lax.axis_index(name) for name in ("z", "y", "x", "c"))
    core_arg = core.astype(jnp.int32).reshape(1)
    tile_odd = ((x + y + z) % 2).astype(jnp.int32).reshape(1)
    pair_odd = (y % 2).astype(jnp.int32).reshape(1)

    position = ((z * NY + y) * 2 + jnp.arange(2)).astype(jnp.float32)
    emphasis = 1.0 + 2.0 * position / 63.0
    strength = emphasis[:, None] * obs_weight
    misfit_part = 0.5 * jnp.sum(
        strength[:, :, None, None] * departure * departure, axis=(0, 1, 2)
    ).reshape(8, 128)
    choose = jnp.where(
        obs_block[:, :, None] == jnp.arange(8, dtype=jnp.int32), strength[:, :, None], 0.0
    )
    tiles = jnp.einsum("sob,soct->scbt", choose, departure, precision=lax.Precision.HIGHEST)

    sent = call(
        pack_kernel,
        shape(512, 128),
        (pair_odd,),
        tiles,
        coarse_decay,
        scratch=[pltpu.VMEM((512, 128), jnp.float32)],
    )
    got = lax.all_to_all(sent.reshape(CHIPS, 4, 128), ZYX, 0, 0).reshape(512, 128)
    other = lax.ppermute(got, "c", SIBLING)

    field = shape(FIELDS, LONS, 8, 128)
    both = shape(2, FIELDS, LONS, 8, 128)
    square = pltpu.VMEM((128, 128), jnp.float32)
    first, second, carry, decay, power = call(
        open_kernel, (field, field, field, field, both), (core_arg,), got, other, scratch=[square]
    )
    zeros, aboves = [], []
    for _ in range(ITERS):
        carry = lax.ppermute(carry, "c", SIBLING)
        zero, above = call(
            close_kernel, (field, both), (core_arg,), first, second, carry, power
        )
        zeros.append(zero)
        aboves.append(above)
        side_even = lax.ppermute(above, ZYX, swap_pairs(0))
        side_odd = lax.ppermute(above, ZYX, swap_pairs(1))
        first, second, carry = call(
            fine_kernel,
            (field, field, field),
            (tile_odd,),
            above,
            side_even,
            side_odd,
            decay,
            scratch=[pltpu.VMEM((FIELDS, 24, 8, 128), jnp.float32)],
        )
    carry = lax.ppermute(carry, "c", SIBLING)
    mine, away = call(
        finish_kernel,
        (shape(256, 128), shape(256, 128)),
        (core_arg,),
        *zeros,
        *aboves,
        first,
        second,
        carry,
        power,
        misfit_part,
        scratch=[square, square],
    )
    other = lax.ppermute(away, "c", SIBLING)
    back = call(join_kernel, shape(512, 128), (core_arg,), mine, other)
    home = lax.all_to_all(back.reshape(CHIPS, 4, 128), ZYX, 0, 0).reshape(512, 128)
    adjoint, misfit, changes = call(
        unpack_kernel,
        (
            jax.ShapeDtypeStruct((2, FIELDS, 8, 1024), jnp.float32),
            jax.ShapeDtypeStruct((1, 1), jnp.float32),
            jax.ShapeDtypeStruct((1, ITERS), jnp.float32),
        ),
        (),
        home,
        scratch=[square],
    )
    return adjoint, misfit.reshape(()), changes.reshape(ITERS)


def solution(mesh):
    split = Mesh(mesh.devices.reshape(NZ, NY, NX, 2), ("z", "y", "x", "c"))
    return jax.shard_map(
        per_device,
        mesh=split,
        in_specs=(P(TM, GRID, None, None), P(TM, GRID), P(TM, GRID), P(None, GRID, None)),
        out_specs=(P(TM, None, GRID, None), P(), P()),
        check_vma=False,
    )
```

```python
import functools

import jax
import jax.numpy as jnp
from jax import lax
from jax.experimental import pallas as pl
from jax.experimental.pallas import tpu as pltpu
from jax.sharding import Mesh
from jax.sharding import PartitionSpec as P

STEPS = 4
ITERS = 3
NZ, NY, NX = 8, 4, 4
CHIPS = NZ * NY * NX
LONS = 8
FIELDS = 3
TM = ("z", "y")
GRID = ("x", "c")
ZYX = ("z", "y", "x")
ALL = ("z", "y", "x", "c")

wave_coef = 0.6
diffusion = 0.05
coriolis = 0.1
epsilon = 1e-06


def chip_of(tile):
    z, place = divmod(tile, NY * NX)
    if z % 2:
        place = NY * NX - 1 - place
    y, x = divmod(place, NX)
    if y % 2:
        x = NX - 1 - x
    return (z * NY + y) * NX + x


def swap_pairs(first):
    pairs = []
    for tile in range(CHIPS):
        core = (tile + first) % 2
        a, b = 2 * chip_of(tile) + core, 2 * chip_of((tile + 1) % CHIPS) + core
        pairs += [(a, b), (b, a)]
    return pairs


SIBLING = [(0, 1), (1, 0)]


def shape(*dims):
    return pltpu.VMEM(dims, jnp.float32)


def near(value):
    return pltpu.with_memory_space_constraint(value, pltpu.VMEM)


def call(kernel, outs, scalars, *operands, far=(), far_out=(), scratch=()):
    vmem = pl.BlockSpec(memory_space=pltpu.VMEM)
    hbm = pl.BlockSpec(memory_space=pl.ANY)
    smem = pl.BlockSpec(memory_space=pltpu.SMEM)
    outs = outs if isinstance(outs, tuple) else (outs,)
    results = pl.pallas_call(
        kernel,
        out_shape=outs,
        in_specs=[smem] * len(scalars) + [hbm] * len(far) + [vmem] * len(operands),
        out_specs=[hbm if i in far_out else vmem for i in range(len(outs))],
        scratch_shapes=list(scratch),
    )(*scalars, *far, *map(near, operands))
    return results if len(outs) > 1 else results[0]


def iota(dim):
    return lax.broadcasted_iota(jnp.int32, (8, 128), dim)


def pack_kernel(
    place_ref,
    departure_ref,
    weight_ref,
    block_ref,
    decay_ref,
    out_ref,
    values_ref,
    weights_ref,
    blocks_ref,
    decays_ref,
    rows_ref,
    sems,
):
    copies = [
        pltpu.make_async_copy(weight_ref, weights_ref, sems.at[0]),
        pltpu.make_async_copy(block_ref, blocks_ref, sems.at[1]),
        pltpu.make_async_copy(decay_ref, decays_ref, sems.at[2]),
    ]
    parts = {
        (j, f): pltpu.make_async_copy(
            departure_ref.at[j, f], values_ref.at[j, f], sems.at[3 + FIELDS * j + f]
        )
        for j in range(2)
        for f in range(FIELDS)
    }
    for copy in copies[:2] + list(parts.values()) + copies[2:]:
        copy.start()
    copies[0].wait()
    copies[1].wait()
    block = lax.broadcasted_iota(jnp.int32, (8, 16), 0)
    for j in range(2):
        emphasis = 1.0 + 2.0 * (place_ref[0] * 2 + j).astype(jnp.float32) / 63.0
        choose = jnp.where(
            blocks_ref[j : j + 1, :] == block, emphasis * weights_ref[j : j + 1, :], 0.0
        )
        for f in range(FIELDS):
            parts[j, f].wait()
            tiles = jnp.dot(
                choose,
                values_ref[j, f],
                precision=lax.Precision.HIGHEST,
                preferred_element_type=jnp.float32,
            )
            for r in range(8):
                rows_ref[pl.ds(24 * j + 8 * f + r, 8, stride=64), :] = tiles[
                    :, 128 * r : 128 * r + 128
                ]
    copies[2].wait()
    odd = (place_ref[0] & 1) == 1
    for b in range(8):
        span = slice(128 * b, 128 * b + 128)
        rows_ref[64 * b + 48 : 64 * b + 56, :] = jnp.where(
            odd, decays_ref[2, :, span], decays_ref[0, :, span]
        )
        rows_ref[64 * b + 56 : 64 * b + 64, :] = decays_ref[1, :, span]
    for b in range(8):
        block = rows_ref[64 * b : 64 * b + 64, :]
        both = jnp.concatenate([block, pltpu.roll(block, 124, 1)], axis=0)
        turned = both.T
        for i in range(16):
            to = 4 * chip_of(16 * b + i)
            out_ref[to : to + 4, :] = turned[8 * i : 8 * i + 4, :]


def later(value, groups):
    return pltpu.roll(value, 128 - 8 * groups, value.ndim - 1)


def scan_pairs(u, square, pair):
    factor = square
    for groups in (1, 2, 4, 8):
        u = u + jnp.where(pair < 16 - groups, factor, 0.0) * later(u, groups)
        factor = factor * factor
    return u


def chain_here(c0, c1, decay, pair, first_ref, second_ref, carry_ref, at):
    square = decay * decay
    value = scan_pairs(c0 + decay * c1, square, pair)
    first_ref[at] = value
    second_ref[at] = c1 + decay * jnp.where(pair < 15, later(value, 1), 0.0)
    spread = jnp.where(pair < 1, value, 0.0)
    for groups in (1, 2, 4, 8):
        spread = spread + pltpu.roll(spread, 8 * groups, spread.ndim - 1)
    carry_ref[at] = spread


def open_kernel(
    core_ref, mine_ref, other_ref, first_ref, second_ref, carry_ref, decay_ref, power_ref, turn_ref
):
    low = core_ref[0] == 0
    lane = iota(1)
    pair = lane // 8
    even = (pair & 1) == 0
    for s in range(4):
        kept, got = (
            jnp.where(low, ref[pl.ds(s, 64, stride=4), :], ref[pl.ds(256 + s, 64, stride=4), :])
            for ref in (mine_ref, other_ref)
        )
        turn_ref[pl.ds(0, 64, stride=2), :] = jnp.where(low, kept, got)
        turn_ref[pl.ds(1, 64, stride=2), :] = jnp.where(low, got, kept)
        turned = turn_ref[...].T
        for half in range(2):
            at = 64 * half
            col = s + 4 * half
            mixed = turned[at + 48 : at + 56, :]
            decays = (
                jnp.where(even, mixed, pltpu.roll(mixed, 8, 1)),
                turned[at + 56 : at + 64, :],
                jnp.where(even, pltpu.roll(mixed, 120, 1), mixed),
            )
            for f in range(FIELDS):
                decay = decays[f]
                c0 = turned[at + 8 * f : at + 8 * f + 8, :]
                c1 = turned[at + 24 + 8 * f : at + 32 + 8 * f, :]
                decay_ref[f, col] = decay
                chain_here(c0, c1, decay, pair, first_ref, second_ref, carry_ref, (f, col))
                power = decay * decay
                for groups in (1, 2, 4, 8):
                    power = power * jnp.where(pair < 16 - groups, later(power, groups), 1.0)
                power_ref[0, f, col] = power
                power_ref[1, f, col] = decay * jnp.where(pair < 15, later(power, 1), 1.0)


def close_kernel(core_ref, first_ref, second_ref, carry_ref, power_ref, zero_ref, above_ref):
    low = core_ref[0] == 0
    pair = iota(1) // 8
    for f in range(FIELDS):
        for col in range(LONS):
            carry = jnp.where(low, carry_ref[f, col], 0.0)
            value = first_ref[f, col] + power_ref[0, f, col] * carry
            zero_ref[f, col] = value
            above_ref[0, f, col] = second_ref[f, col] + power_ref[1, f, col] * carry
            above_ref[1, f, col] = jnp.where(pair < 15, later(value, 1), carry)


def fine_kernel(
    odd_ref, own_ref, even_ref, odd_side_ref, decay_ref, first_ref, second_ref, carry_ref, state_ref
):
    odd = odd_ref[0] == 1
    row = iota(0)[None]
    lane = iota(1)[None]
    band = lane % 8
    pair = lane // 8
    at_top = row == 0
    at_end = row == 7
    not_first = band > 0
    not_last = band < 7

    def next_row(v):
        inner = pltpu.roll(v, 7, 1)
        edge = jnp.where(not_last, pltpu.roll(inner, 127, 2), 0.0)
        return jnp.where(at_end, edge, inner)

    def last_row(v):
        inner = pltpu.roll(v, 1, 1)
        edge = jnp.where(not_first, pltpu.roll(inner, 1, 2), 0.0)
        return jnp.where(at_top, edge, inner)

    corrections = []
    for j in range(2):
        for f in range(FIELDS):
            one, two = even_ref[j, f], odd_side_ref[j, f]
            state_ref[f, 0:8] = jnp.where(odd, one, two)
            state_ref[f, 8:16] = own_ref[j, f]
            state_ref[f, 16:24] = jnp.where(odd, two, one)
        p, q, r = state_ref[0], state_ref[1], state_ref[2]
        keep = 1.0 / diffusion - 4.0
        wave = 0.5 * wave_coef / diffusion
        wave_new = 0.5 * wave_coef
        turn = coriolis / diffusion
        for step in range(STEPS):
            n = p.shape[0]
            pc, rc = p[1 : n - 1], r[1 : n - 1]
            side = wave * rc
            p1 = (
                (keep * pc + (p[: n - 2] + p[2:]))
                + wave * (q[2:] - q[: n - 2])
                + (next_row(pc + side) + last_row(pc - side))
            )
            qc, rc, pc = q[2 : n - 2], r[2 : n - 2], p1[1 : n - 3]
            push = wave_new * p1
            side = push[1 : n - 3]
            q1 = (
                (keep * qc + (q[1 : n - 3] + q[3 : n - 1]))
                + ((push[2:] - push[: n - 4]) + turn * rc)
                + (next_row(qc) + last_row(qc))
            )
            r1 = (
                (keep * rc + (r[1 : n - 3] + r[3 : n - 1]))
                - turn * qc
                + (next_row(rc + side) + last_row(rc - side))
            )
            p, q, r = pc, q1, r1
        unit = diffusion**STEPS
        corrections.append([unit * v - decay_ref[f] * own_ref[j, f] for f, v in enumerate((p, q, r))])
    for f in range(FIELDS):
        chain_here(
            corrections[0][f], corrections[1][f], decay_ref[f], pair, first_ref, second_ref, carry_ref, f
        )


def finish_kernel(core_ref, *refs):
    zeros = refs[0:3]
    aboves = refs[3:6]
    first_ref, second_ref, carry_ref, power_ref, misfit_ref = refs[6:11]
    mine_ref, other_ref, turn_ref, back_ref = refs[11:]
    low = core_ref[0] == 0
    pair = iota(1) // 8
    subwindow = (2 * (pair + jnp.where(low, 0, 16))).astype(jnp.float32)
    emphasis = [1.0 + 2.0 * (subwindow + j) / 63.0 for j in range(2)]
    sums = [jnp.zeros((8, 128), jnp.float32) for _ in range(2 * ITERS)]
    result = {}
    for f in range(FIELDS):
        for col in range(LONS):
            carry = jnp.where(low, carry_ref[f, col], 0.0)
            last = (
                first_ref[f, col] + power_ref[0, f, col] * carry,
                second_ref[f, col] + power_ref[1, f, col] * carry,
            )
            for j in range(2):
                so_far = zeros[0][f, col] if j == 0 else aboves[0][0, f, col]
                for n in range(ITERS):
                    if n == ITERS - 1:
                        change = last[j]
                    else:
                        change = zeros[n + 1][f, col] if j == 0 else aboves[n + 1][0, f, col]
                    so_far = so_far + change
                    sums[n] = sums[n] + emphasis[j] * (change * change)
                    sums[ITERS + n] = sums[ITERS + n] + emphasis[j] * (so_far * so_far)
                result[j, f, col] = so_far
    row = iota(0)
    parts = jnp.zeros((8, 128), jnp.float32)
    for at, part in enumerate(sums[:ITERS] + [misfit_ref[...]] + sums[ITERS:]):
        parts = jnp.where(row == at, jnp.sum(part, axis=0, keepdims=True), parts)
    ones = jnp.ones((128, 128), jnp.float32)
    totals = jnp.dot(parts, ones, precision=lax.Precision.HIGHEST)
    turn_ref[48:56, :] = totals
    for s in range(4):
        for half in range(2):
            at = 64 * half
            for j in range(2):
                for f in range(FIELDS):
                    to = at + 24 * j + 8 * f
                    turn_ref[to : to + 8, :] = result[j, f, s + 4 * half]
        back_ref[...] = turn_ref[...].T
        evens = back_ref[pl.ds(0, 64, stride=2), :]
        odds = back_ref[pl.ds(1, 64, stride=2), :]
        mine_ref[pl.ds(s, 64, stride=4), :] = jnp.where(low, evens, odds)
        other_ref[pl.ds(s, 64, stride=4), :] = jnp.where(low, odds, evens)


def join_kernel(core_ref, mine_ref, got_ref, out_ref):
    low = core_ref[0] == 0
    lane = lax.broadcasted_iota(jnp.int32, (256, 128), 1)
    counted = (lane & 120) == 48
    mine, got = mine_ref[...], got_ref[...]
    total = mine + got
    out_ref[0:256, :] = jnp.where(counted, total, jnp.where(low, mine, got))
    out_ref[256:512, :] = jnp.where(counted, total, jnp.where(low, got, mine))


def unpack_kernel(in_ref, out_ref, misfit_ref, changes_ref, rows_ref, stage_ref, sems):
    sums = [in_ref[8 * v : 8 * v + 8, :] for v in range(64)]
    while len(sums) > 1:
        sums = [a + b for a, b in zip(sums[::2], sums[1::2])]
    total = pltpu.roll(sums[0] + pltpu.roll(sums[0], 4, 0), 80, 1)
    misfit_ref[...] = total[0:1, 3:4]
    changes_ref[...] = (total / (pltpu.roll(total, 124, 1) + epsilon))[0:1, 0:ITERS]
    second = (lax.broadcasted_iota(jnp.int32, (128, 128), 0) & 7) >= 4
    copies = []
    for b in range(8):
        for i in range(16):
            at = 4 * chip_of(16 * b + i)
            piece = in_ref[at : at + 4, :]
            rows_ref[8 * i : 8 * i + 4, :] = piece
            rows_ref[8 * i + 4 : 8 * i + 8, :] = piece
        block = rows_ref[...]
        turned = jnp.where(second, pltpu.roll(block, 64, 1), block).T
        for j in range(2):
            for f in range(FIELDS):
                at = 24 * j + 8 * f
                stage_ref[b, j, f] = turned[at : at + 8, :]
        copies.append(
            pltpu.make_async_copy(
                stage_ref.at[b], out_ref.at[:, :, :, 128 * b : 128 * b + 128], sems.at[b]
            )
        )
        copies[-1].start()
    for copy in copies:
        copy.wait()


def per_device(departure, obs_weight, obs_block, coarse_decay):
    z, y, x, core = (lax.axis_index(name) for name in ("z", "y", "x", "c"))
    core_arg = core.astype(jnp.int32).reshape(1)
    tile_odd = ((x + y + z + core) % 2).astype(jnp.int32).reshape(1)
    place = (z * NY + y).astype(jnp.int32).reshape(1)

    position = ((z * NY + y) * 2 + jnp.arange(2)).astype(jnp.float32)
    strength = (1.0 + 2.0 * position / 63.0)[:, None] * obs_weight
    misfit_part = 0.5 * jnp.sum(
        strength[:, :, None, None] * departure * departure, axis=(0, 1, 2)
    ).reshape(8, 128)

    sent = call(
        pack_kernel,
        shape(512, 128),
        (place,),
        far=(departure.transpose(0, 2, 1, 3), obs_weight, obs_block, coarse_decay),
        scratch=[
            pltpu.VMEM((2, FIELDS, 16, 1024), jnp.float32),
            pltpu.VMEM((2, 16), jnp.float32),
            pltpu.VMEM((2, 16), jnp.int32),
            pltpu.VMEM((FIELDS, 8, 1024), jnp.float32),
            pltpu.VMEM((512, 128), jnp.float32),
            pltpu.SemaphoreType.DMA((9,)),
        ],
    )
    got = lax.all_to_all(sent.reshape(CHIPS, 4, 128), ZYX, 0, 0).reshape(512, 128)
    other = lax.ppermute(got, "c", SIBLING)

    field = shape(FIELDS, LONS, 8, 128)
    both = shape(2, FIELDS, LONS, 8, 128)
    square = pltpu.VMEM((128, 128), jnp.float32)
    first, second, carry, decay, power = call(
        open_kernel, (field, field, field, field, both), (core_arg,), got, other, scratch=[square]
    )
    zeros, aboves = [], []
    for _ in range(ITERS):
        carry = lax.ppermute(carry, "c", SIBLING)
        zero, above = call(
            close_kernel, (field, both), (core_arg,), first, second, carry, power
        )
        zeros.append(zero)
        aboves.append(above)
        side_even = lax.ppermute(above, ALL, swap_pairs(0))
        side_odd = lax.ppermute(above, ALL, swap_pairs(1))
        first, second, carry = call(
            fine_kernel,
            (field, field, field),
            (tile_odd,),
            above,
            side_even,
            side_odd,
            decay,
            scratch=[pltpu.VMEM((FIELDS, 24, 8, 128), jnp.float32)],
        )
    carry = lax.ppermute(carry, "c", SIBLING)
    mine, away = call(
        finish_kernel,
        (shape(256, 128), shape(256, 128)),
        (core_arg,),
        *zeros,
        *aboves,
        first,
        second,
        carry,
        power,
        misfit_part,
        scratch=[square, square],
    )
    other = lax.ppermute(away, "c", SIBLING)
    back = call(join_kernel, shape(512, 128), (core_arg,), mine, other)
    home = lax.all_to_all(back.reshape(CHIPS, 4, 128), ZYX, 0, 0).reshape(512, 128)
    adjoint, misfit, changes = call(
        unpack_kernel,
        (
            jax.ShapeDtypeStruct((2, FIELDS, 8, 1024), jnp.float32),
            jax.ShapeDtypeStruct((1, 1), jnp.float32),
            jax.ShapeDtypeStruct((1, ITERS), jnp.float32),
        ),
        (),
        home,
        far_out=(0,),
        scratch=[
            square,
            pltpu.VMEM((8, 2, FIELDS, 8, 128), jnp.float32),
            pltpu.SemaphoreType.DMA((8,)),
        ],
    )
    return adjoint, misfit.reshape(()), changes.reshape(ITERS)


def solution(mesh):
    split = Mesh(mesh.devices.reshape(NZ, NY, NX, 2), ("z", "y", "x", "c"))
    return jax.shard_map(
        per_device,
        mesh=split,
        in_specs=(P(TM, GRID, None, None), P(TM, GRID), P(TM, GRID), P(None, GRID, None)),
        out_specs=(P(TM, None, GRID, None), P(), P()),
        check_vma=False,
    )
```

```python
import functools

import jax
import jax.numpy as jnp
from jax import lax
from jax.experimental import pallas as pl
from jax.experimental.pallas import tpu as pltpu
from jax.sharding import Mesh
from jax.sharding import PartitionSpec as P

STEPS = 4
ITERS = 3
NZ, NY, NX = 8, 4, 4
CHIPS = NZ * NY * NX
LONS = 8
FIELDS = 3
TM = ("z", "y")
GRID = ("x", "c")
ZYX = ("z", "y", "x")
ALL = ("z", "y", "x", "c")

wave_coef = 0.6
diffusion = 0.05
coriolis = 0.1
epsilon = 1e-06


def chip_of(tile):
    z, place = divmod(tile, NY * NX)
    if z % 2:
        place = NY * NX - 1 - place
    y, x = divmod(place, NX)
    if y % 2:
        x = NX - 1 - x
    return (z * NY + y) * NX + x


def swap_pairs(first):
    pairs = []
    for tile in range(CHIPS):
        core = (tile + first) % 2
        a, b = 2 * chip_of(tile) + core, 2 * chip_of((tile + 1) % CHIPS) + core
        pairs += [(a, b), (b, a)]
    return pairs


SIBLING = [(0, 1), (1, 0)]


def shape(*dims):
    return pltpu.VMEM(dims, jnp.float32)


def near(value):
    return pltpu.with_memory_space_constraint(value, pltpu.VMEM)


def call(kernel, outs, scalars, *operands, far=(), scratch=()):
    vmem = pl.BlockSpec(memory_space=pltpu.VMEM)
    hbm = pl.BlockSpec(memory_space=pl.ANY)
    smem = pl.BlockSpec(memory_space=pltpu.SMEM)
    outs = outs if isinstance(outs, tuple) else (outs,)
    results = pl.pallas_call(
        kernel,
        out_shape=outs,
        in_specs=[smem] * len(scalars) + [hbm] * len(far) + [vmem] * len(operands),
        out_specs=[vmem] * len(outs),
        scratch_shapes=list(scratch),
    )(*scalars, *far, *map(near, operands))
    return results if len(outs) > 1 else results[0]


def iota(dim):
    return lax.broadcasted_iota(jnp.int32, (8, 128), dim)


def pack_kernel(
    place_ref,
    departure_ref,
    weight_ref,
    block_ref,
    decay_ref,
    out_ref,
    values_ref,
    weights_ref,
    blocks_ref,
    decays_ref,
    rows_ref,
    sems,
):
    copies = [
        pltpu.make_async_copy(weight_ref, weights_ref, sems.at[0]),
        pltpu.make_async_copy(block_ref, blocks_ref, sems.at[1]),
        pltpu.make_async_copy(decay_ref, decays_ref, sems.at[2]),
    ]
    parts = {
        (j, f): pltpu.make_async_copy(
            departure_ref.at[j, f], values_ref.at[j, f], sems.at[3 + FIELDS * j + f]
        )
        for j in range(2)
        for f in range(FIELDS)
    }
    for copy in copies[:2] + list(parts.values()) + copies[2:]:
        copy.start()
    copies[0].wait()
    copies[1].wait()
    block = lax.broadcasted_iota(jnp.int32, (8, 16), 0)
    for j in range(2):
        emphasis = 1.0 + 2.0 * (place_ref[0] * 2 + j).astype(jnp.float32) / 63.0
        choose = jnp.where(
            blocks_ref[j : j + 1, :] == block, emphasis * weights_ref[j : j + 1, :], 0.0
        )
        for f in range(FIELDS):
            parts[j, f].wait()
            tiles = jnp.dot(
                choose,
                values_ref[j, f],
                precision=lax.Precision.HIGHEST,
                preferred_element_type=jnp.float32,
            )
            for r in range(8):
                rows_ref[pl.ds(24 * j + 8 * f + r, 8, stride=64), :] = tiles[
                    :, 128 * r : 128 * r + 128
                ]
    copies[2].wait()
    odd = (place_ref[0] & 1) == 1
    for b in range(8):
        span = slice(128 * b, 128 * b + 128)
        rows_ref[64 * b + 48 : 64 * b + 56, :] = jnp.where(
            odd, decays_ref[2, :, span], decays_ref[0, :, span]
        )
        rows_ref[64 * b + 56 : 64 * b + 64, :] = decays_ref[1, :, span]
    for b in range(8):
        block = rows_ref[64 * b : 64 * b + 64, :]
        both = jnp.concatenate([block, pltpu.roll(block, 124, 1)], axis=0)
        turned = both.T
        for i in range(16):
            to = 4 * chip_of(16 * b + i)
            out_ref[to : to + 4, :] = turned[8 * i : 8 * i + 4, :]


def later(value, groups):
    return pltpu.roll(value, 128 - 8 * groups, value.ndim - 1)


def scan_pairs(u, square, pair):
    for groups in (1, 4):
        factor = square
        total = u
        for times in (1, 2, 3):
            back = times * groups
            total = total + jnp.where(pair < 16 - back, factor, 0.0) * later(u, back)
            factor = factor * square
        u, square = total, factor
    return u


def chain_here(terms, first_ref, second_ref, carry_ref):
    pair = iota(1) // 8
    for f in range(FIELDS):
        for col in range(LONS):
            c0, c1, decay = terms(f, col)
            value = scan_pairs(c0 + decay * c1, decay * decay, pair)
            first_ref[f, col] = value
            second_ref[f, col] = c1 + decay * jnp.where(pair < 15, later(value, 1), 0.0)
    source = lax.broadcasted_iota(jnp.int32, (128, 128), 0)
    target = lax.broadcasted_iota(jnp.int32, (128, 128), 1)
    spread = (source == target % 8).astype(jnp.float32)
    values = first_ref[...].reshape(FIELDS * LONS * 8, 128)
    carried = jnp.dot(
        values, spread, precision=lax.Precision.HIGHEST, preferred_element_type=jnp.float32
    )
    carry_ref[...] = carried.reshape(FIELDS, LONS, 8, 128)


def powers(square, exponent):
    power = jnp.where((exponent & 1) != 0, square, 1.0)
    for bit in (2, 4, 8, 16):
        square = square * square
        power = power * jnp.where((exponent & bit) != 0, square, 1.0)
    return power


def open_kernel(
    core_ref, mine_ref, other_ref, first_ref, second_ref, carry_ref, decay_ref, power_ref, turn_ref, terms_ref
):
    low = core_ref[0] == 0
    lane = iota(1)
    pair = lane // 8
    even = (pair & 1) == 0
    for s in range(4):
        kept, got = (
            jnp.where(low, ref[pl.ds(s, 64, stride=4), :], ref[pl.ds(256 + s, 64, stride=4), :])
            for ref in (mine_ref, other_ref)
        )
        turn_ref[pl.ds(0, 64, stride=2), :] = jnp.where(low, kept, got)
        turn_ref[pl.ds(1, 64, stride=2), :] = jnp.where(low, got, kept)
        turned = turn_ref[...].T
        for half in range(2):
            at = 64 * half
            col = s + 4 * half
            mixed = turned[at + 48 : at + 56, :]
            decays = (
                jnp.where(even, mixed, pltpu.roll(mixed, 8, 1)),
                turned[at + 56 : at + 64, :],
                jnp.where(even, pltpu.roll(mixed, 120, 1), mixed),
            )
            for f in range(FIELDS):
                decay = decays[f]
                decay_ref[f, col] = decay
                terms_ref[0, f, col] = turned[at + 8 * f : at + 8 * f + 8, :]
                terms_ref[1, f, col] = turned[at + 24 + 8 * f : at + 32 + 8 * f, :]
                square = decay * decay
                power_ref[0, f, col] = powers(square, 16 - pair)
                power_ref[1, f, col] = decay * powers(square, 15 - pair)
    chain_here(
        lambda f, col: (terms_ref[0, f, col], terms_ref[1, f, col], decay_ref[f, col]),
        first_ref,
        second_ref,
        carry_ref,
    )


def close_kernel(core_ref, first_ref, second_ref, carry_ref, power_ref, zero_ref, above_ref):
    low = core_ref[0] == 0
    pair = iota(1) // 8
    for f in range(FIELDS):
        for col in range(LONS):
            carry = jnp.where(low, carry_ref[f, col], 0.0)
            value = first_ref[f, col] + power_ref[0, f, col] * carry
            zero_ref[f, col] = value
            above_ref[0, f, col] = second_ref[f, col] + power_ref[1, f, col] * carry
            above_ref[1, f, col] = jnp.where(pair < 15, later(value, 1), carry)


def fine_kernel(
    odd_ref, own_ref, one_ref, two_ref, decay_ref, first_ref, second_ref, carry_ref, state_ref
):
    odd = odd_ref[0] == 1
    lane = iota(1)
    band = lane % 8
    width = 3 * LONS

    def slot(j, f, col):
        return 24 * ((j * FIELDS + f) * width + col)

    def put(j, f, col, value):
        at = slot(j, f, col) + 8
        state_ref[at : at + 8, :] = value

    def here(j, f, col):
        at = slot(j, f, col) + 8
        return state_ref[at : at + 8, :]

    def rows(j, f, col):
        at = slot(j, f, col) + 8
        return state_ref[at + 1 : at + 9, :], state_ref[at - 1 : at + 7, :]

    def edges(j, f, low, high):
        for col in range(low, high, 8):
            at = slot(j, f, min(col, width - 8))
            first = pltpu.roll(state_ref[pl.ds(at + 8, 8, stride=24), :], 127, 1)
            last = pltpu.roll(state_ref[pl.ds(at + 15, 8, stride=24), :], 1, 1)
            state_ref[pl.ds(at + 16, 8, stride=24), :] = jnp.where(band < 7, first, 0.0)
            state_ref[pl.ds(at + 7, 8, stride=24), :] = jnp.where(band > 0, last, 0.0)

    for j in range(2):
        for f in range(FIELDS):
            for at in range(LONS):
                one, two = one_ref[j, f, at], two_ref[j, f, at]
                put(j, f, at, jnp.where(odd, one, two))
                put(j, f, LONS + at, own_ref[j, f, at])
                put(j, f, 2 * LONS + at, jnp.where(odd, two, one))
            edges(j, f, 0, width)

    keep = 1.0 / diffusion - 4.0
    wave = 0.5 * wave_coef / diffusion
    wave_new = 0.5 * wave_coef
    turn = coriolis / diffusion
    unit = diffusion**STEPS
    result = {}
    for step in range(STEPS):
        low, high = 2 * step + 1, width - 2 * step - 1
        for j in range(2):
            p = {col: here(j, 0, col) for col in (low - 1, low)}
            q = {col: here(j, 1, col) for col in (low - 1, low)}
            for col in range(low, high):
                p[col + 1], q[col + 1] = here(j, 0, col + 1), here(j, 1, col + 1)
                p_next, p_last = rows(j, 0, col)
                r_next, r_last = rows(j, 2, col)
                p1 = ((keep * p[col] + (p[col - 1] + p[col + 1])) + (p_next + p_last)) + wave * (
                    (q[col + 1] - q[col - 1]) + (r_next - r_last)
                )
                put(j, 0, col, p1)
            edges(j, 0, low, high)
        low, high = low + 1, high - 1
        for j in range(2):
            p, q, r = (
                {col: here(j, f, col) for col in (low - 1, low)} for f in range(FIELDS)
            )
            for col in range(low, high):
                p[col + 1], q[col + 1], r[col + 1] = (here(j, f, col + 1) for f in range(FIELDS))
                p_next, p_last = rows(j, 0, col)
                q_next, q_last = rows(j, 1, col)
                r_next, r_last = rows(j, 2, col)
                q1 = (
                    (keep * q[col] + (q[col - 1] + q[col + 1])) + (q_next + q_last)
                ) + (wave_new * (p[col + 1] - p[col - 1]) + turn * r[col])
                r1 = (
                    (keep * r[col] + (r[col - 1] + r[col + 1])) + (r_next + r_last)
                ) + (wave_new * (p_next - p_last) - turn * q[col])
                if step < STEPS - 1:
                    put(j, 1, col, q1)
                    put(j, 2, col, r1)
                else:
                    for f, value in enumerate((p[col], q1, r1)):
                        result[j, f, col - LONS] = value
            if step < STEPS - 1:
                edges(j, 1, low, high)
                edges(j, 2, low, high)

    def terms(f, col):
        decay = decay_ref[f, col]
        return *(unit * result[j, f, col] - decay * own_ref[j, f, col] for j in range(2)), decay

    chain_here(terms, first_ref, second_ref, carry_ref)


def finish_kernel(core_ref, *refs):
    zeros = refs[0:3]
    aboves = refs[3:6]
    first_ref, second_ref, carry_ref, power_ref, misfit_ref = refs[6:11]
    mine_ref, other_ref, turn_ref, back_ref = refs[11:]
    low = core_ref[0] == 0
    pair = iota(1) // 8
    subwindow = (2 * (pair + jnp.where(low, 0, 16))).astype(jnp.float32)
    emphasis = [1.0 + 2.0 * (subwindow + j) / 63.0 for j in range(2)]
    sums = [jnp.zeros((8, 128), jnp.float32) for _ in range(2 * ITERS)]
    result = {}
    for f in range(FIELDS):
        for col in range(LONS):
            carry = jnp.where(low, carry_ref[f, col], 0.0)
            last = (
                first_ref[f, col] + power_ref[0, f, col] * carry,
                second_ref[f, col] + power_ref[1, f, col] * carry,
            )
            for j in range(2):
                so_far = zeros[0][f, col] if j == 0 else aboves[0][0, f, col]
                for n in range(ITERS):
                    if n == ITERS - 1:
                        change = last[j]
                    else:
                        change = zeros[n + 1][f, col] if j == 0 else aboves[n + 1][0, f, col]
                    so_far = so_far + change
                    sums[n] = sums[n] + emphasis[j] * (change * change)
                    sums[ITERS + n] = sums[ITERS + n] + emphasis[j] * (so_far * so_far)
                result[j, f, col] = so_far
    row = iota(0)
    parts = jnp.zeros((8, 128), jnp.float32)
    for at, part in enumerate(sums[:ITERS] + [misfit_ref[...]] + sums[ITERS:]):
        parts = jnp.where(row == at, jnp.sum(part, axis=0, keepdims=True), parts)
    ones = jnp.ones((128, 128), jnp.float32)
    totals = jnp.dot(parts, ones, precision=lax.Precision.HIGHEST)
    turn_ref[48:56, :] = totals
    for s in range(4):
        for half in range(2):
            at = 64 * half
            for j in range(2):
                for f in range(FIELDS):
                    to = at + 24 * j + 8 * f
                    turn_ref[to : to + 8, :] = result[j, f, s + 4 * half]
        back_ref[...] = turn_ref[...].T
        evens = back_ref[pl.ds(0, 64, stride=2), :]
        odds = back_ref[pl.ds(1, 64, stride=2), :]
        mine_ref[pl.ds(s, 64, stride=4), :] = jnp.where(low, evens, odds)
        other_ref[pl.ds(s, 64, stride=4), :] = jnp.where(low, odds, evens)


def join_kernel(core_ref, mine_ref, got_ref, out_ref):
    low = core_ref[0] == 0
    lane = lax.broadcasted_iota(jnp.int32, (256, 128), 1)
    counted = (lane & 120) == 48
    mine, got = mine_ref[...], got_ref[...]
    total = mine + got
    out_ref[0:256, :] = jnp.where(counted, total, jnp.where(low, mine, got))
    out_ref[256:512, :] = jnp.where(counted, total, jnp.where(low, got, mine))


def unpack_kernel(in_ref, out_ref, misfit_ref, changes_ref, rows_ref):
    sums = [in_ref[8 * v : 8 * v + 8, :] for v in range(64)]
    while len(sums) > 1:
        sums = [a + b for a, b in zip(sums[::2], sums[1::2])]
    total = pltpu.roll(sums[0] + pltpu.roll(sums[0], 4, 0), 80, 1)
    misfit_ref[...] = total[0:1, 3:4]
    changes_ref[...] = (total / (pltpu.roll(total, 124, 1) + epsilon))[0:1, 0:ITERS]
    second = (lax.broadcasted_iota(jnp.int32, (128, 128), 0) & 7) >= 4
    for b in range(8):
        for i in range(16):
            at = 4 * chip_of(16 * b + i)
            piece = in_ref[at : at + 4, :]
            rows_ref[8 * i : 8 * i + 4, :] = piece
            rows_ref[8 * i + 4 : 8 * i + 8, :] = piece
        block = rows_ref[...]
        turned = jnp.where(second, pltpu.roll(block, 64, 1), block).T
        for j in range(2):
            for f in range(FIELDS):
                at = 24 * j + 8 * f
                out_ref[j, f, :, 128 * b : 128 * b + 128] = turned[at : at + 8, :]


def per_device(departure, obs_weight, obs_block, coarse_decay):
    z, y, x, core = (lax.axis_index(name) for name in ("z", "y", "x", "c"))
    core_arg = core.astype(jnp.int32).reshape(1)
    tile_odd = ((x + y + z + core) % 2).astype(jnp.int32).reshape(1)
    place = (z * NY + y).astype(jnp.int32).reshape(1)

    position = ((z * NY + y) * 2 + jnp.arange(2)).astype(jnp.float32)
    strength = (1.0 + 2.0 * position / 63.0)[:, None] * obs_weight
    misfit_part = 0.5 * jnp.sum(
        strength[:, :, None, None] * departure * departure, axis=(0, 1, 2)
    ).reshape(8, 128)

    sent = call(
        pack_kernel,
        shape(512, 128),
        (place,),
        far=(departure.transpose(0, 2, 1, 3), obs_weight, obs_block, coarse_decay),
        scratch=[
            pltpu.VMEM((2, FIELDS, 16, 1024), jnp.float32),
            pltpu.VMEM((2, 16), jnp.float32),
            pltpu.VMEM((2, 16), jnp.int32),
            pltpu.VMEM((FIELDS, 8, 1024), jnp.float32),
            pltpu.VMEM((512, 128), jnp.float32),
            pltpu.SemaphoreType.DMA((9,)),
        ],
    )
    got = lax.all_to_all(sent.reshape(CHIPS, 4, 128), ZYX, 0, 0).reshape(512, 128)
    other = lax.ppermute(got, "c", SIBLING)

    field = shape(FIELDS, LONS, 8, 128)
    both = shape(2, FIELDS, LONS, 8, 128)
    square = pltpu.VMEM((128, 128), jnp.float32)
    first, second, carry, decay, power = call(
        open_kernel, (field, field, field, field, both), (core_arg,), got, other, scratch=[square, pltpu.VMEM((2, FIELDS, LONS, 8, 128), jnp.float32)]
    )
    zeros, aboves = [], []
    for _ in range(ITERS):
        carry = lax.ppermute(carry, "c", SIBLING)
        zero, above = call(
            close_kernel, (field, both), (core_arg,), first, second, carry, power
        )
        zeros.append(zero)
        aboves.append(above)
        side_even = lax.ppermute(above, ALL, swap_pairs(0))
        side_odd = lax.ppermute(above, ALL, swap_pairs(1))
        first, second, carry = call(
            fine_kernel,
            (field, field, field),
            (tile_odd,),
            above,
            side_even,
            side_odd,
            decay,
            scratch=[pltpu.VMEM((2 * FIELDS * 3 * LONS * 24, 128), jnp.float32)],
        )
    carry = lax.ppermute(carry, "c", SIBLING)
    mine, away = call(
        finish_kernel,
        (shape(256, 128), shape(256, 128)),
        (core_arg,),
        *zeros,
        *aboves,
        first,
        second,
        carry,
        power,
        misfit_part,
        scratch=[square, square],
    )
    other = lax.ppermute(away, "c", SIBLING)
    back = call(join_kernel, shape(512, 128), (core_arg,), mine, other)
    home = lax.all_to_all(back.reshape(CHIPS, 4, 128), ZYX, 0, 0).reshape(512, 128)
    adjoint, misfit, changes = call(
        unpack_kernel,
        (
            jax.ShapeDtypeStruct((2, FIELDS, 8, 1024), jnp.float32),
            jax.ShapeDtypeStruct((1, 1), jnp.float32),
            jax.ShapeDtypeStruct((1, ITERS), jnp.float32),
        ),
        (),
        home,
        scratch=[square],
    )
    return adjoint, misfit.reshape(()), changes.reshape(ITERS)


def solution(mesh):
    split = Mesh(mesh.devices.reshape(NZ, NY, NX, 2), ("z", "y", "x", "c"))
    return jax.shard_map(
        per_device,
        mesh=split,
        in_specs=(P(TM, GRID, None, None), P(TM, GRID), P(TM, GRID), P(None, GRID, None)),
        out_specs=(P(TM, None, GRID, None), P(), P()),
        check_vma=False,
    )
```

```python
import functools

import jax
import jax.numpy as jnp
from jax import lax
from jax.experimental import pallas as pl
from jax.experimental.pallas import tpu as pltpu
from jax.sharding import Mesh
from jax.sharding import PartitionSpec as P

STEPS = 4
ITERS = 3
NZ, NY, NX = 8, 4, 4
CHIPS = NZ * NY * NX
LONS = 8
FIELDS = 3
TM = ("z", "y")
GRID = ("x", "c")
ZYX = ("z", "y", "x")
ALL = ("z", "y", "x", "c")

wave_coef = 0.6
diffusion = 0.05
coriolis = 0.1
epsilon = 1e-06


def chip_of(tile):
    z, place = divmod(tile, NY * NX)
    if z % 2:
        place = NY * NX - 1 - place
    y, x = divmod(place, NX)
    if y % 2:
        x = NX - 1 - x
    return (z * NY + y) * NX + x


def swap_pairs(first):
    pairs = []
    for tile in range(CHIPS):
        core = (tile + first) % 2
        a, b = 2 * chip_of(tile) + core, 2 * chip_of((tile + 1) % CHIPS) + core
        pairs += [(a, b), (b, a)]
    return pairs


SIBLING = [(0, 1), (1, 0)]


def shape(*dims):
    return pltpu.VMEM(dims, jnp.float32)


def near(value):
    return pltpu.with_memory_space_constraint(value, pltpu.VMEM)


def call(kernel, outs, scalars, *operands, far=(), scratch=()):
    vmem = pl.BlockSpec(memory_space=pltpu.VMEM)
    hbm = pl.BlockSpec(memory_space=pl.ANY)
    smem = pl.BlockSpec(memory_space=pltpu.SMEM)
    outs = outs if isinstance(outs, tuple) else (outs,)
    results = pl.pallas_call(
        kernel,
        out_shape=outs,
        in_specs=[smem] * len(scalars) + [hbm] * len(far) + [vmem] * len(operands),
        out_specs=[vmem] * len(outs),
        scratch_shapes=list(scratch),
    )(*scalars, *far, *map(near, operands))
    return results if len(outs) > 1 else results[0]


def iota(dim):
    return lax.broadcasted_iota(jnp.int32, (8, 128), dim)


def pack_kernel(
    place_ref,
    departure_ref,
    weight_ref,
    block_ref,
    decay_ref,
    out_ref,
    values_ref,
    weights_ref,
    blocks_ref,
    decays_ref,
    rows_ref,
    sems,
):
    copies = [
        pltpu.make_async_copy(weight_ref, weights_ref, sems.at[0]),
        pltpu.make_async_copy(block_ref, blocks_ref, sems.at[1]),
        pltpu.make_async_copy(decay_ref, decays_ref, sems.at[2]),
    ]
    parts = {
        (j, f): pltpu.make_async_copy(
            departure_ref.at[j, f], values_ref.at[j, f], sems.at[3 + FIELDS * j + f]
        )
        for j in range(2)
        for f in range(FIELDS)
    }
    for copy in copies[:2] + list(parts.values()) + copies[2:]:
        copy.start()
    copies[0].wait()
    copies[1].wait()
    block = lax.broadcasted_iota(jnp.int32, (8, 16), 0)
    for j in range(2):
        emphasis = 1.0 + 2.0 * (place_ref[0] * 2 + j).astype(jnp.float32) / 63.0
        choose = jnp.where(
            blocks_ref[j : j + 1, :] == block, emphasis * weights_ref[j : j + 1, :], 0.0
        )
        for f in range(FIELDS):
            parts[j, f].wait()
            tiles = jnp.dot(
                choose,
                values_ref[j, f],
                precision=lax.Precision.HIGHEST,
                preferred_element_type=jnp.float32,
            )
            for r in range(8):
                rows_ref[pl.ds(24 * j + 8 * f + r, 8, stride=64), :] = tiles[
                    :, 128 * r : 128 * r + 128
                ]
    copies[2].wait()
    odd = (place_ref[0] & 1) == 1
    for b in range(8):
        span = slice(128 * b, 128 * b + 128)
        rows_ref[64 * b + 48 : 64 * b + 56, :] = jnp.where(
            odd, decays_ref[2, :, span], decays_ref[0, :, span]
        )
        rows_ref[64 * b + 56 : 64 * b + 64, :] = decays_ref[1, :, span]
    for b in range(8):
        block = rows_ref[64 * b : 64 * b + 64, :]
        both = jnp.concatenate([block, pltpu.roll(block, 124, 1)], axis=0)
        turned = both.T
        for i in range(16):
            to = 4 * chip_of(16 * b + i)
            out_ref[to : to + 4, :] = turned[8 * i : 8 * i + 4, :]


def later(value, groups):
    return pltpu.roll(value, 128 - 8 * groups, value.ndim - 1)


def scan_pairs(u, square, pair):
    for groups in (1, 4):
        factor = square
        total = u
        for times in (1, 2, 3):
            back = times * groups
            total = total + jnp.where(pair < 16 - back, factor, 0.0) * later(u, back)
            factor = factor * square
        u, square = total, factor
    return u


def bands_summed(values):
    source = lax.broadcasted_iota(jnp.int32, (128, 128), 0)
    target = lax.broadcasted_iota(jnp.int32, (128, 128), 1)
    same = (source % 8 == target % 8).astype(jnp.float32)
    return jnp.dot(
        values, same, precision=lax.Precision.HIGHEST, preferred_element_type=jnp.float32
    )


def chain_first(terms_of, decay_ref, pairs_ref, carry_ref, weigh_ref):
    pair = iota(1) // 8
    for f in range(FIELDS):
        for col in range(LONS):
            decay = decay_ref[f, col]
            c0, c1 = terms_of(f, col)
            both = c0 + decay * c1
            if pairs_ref is not None:
                pairs_ref[0, f, col] = both
                pairs_ref[1, f, col] = c1
            at = 8 * (LONS * f + col)
            weigh_ref[at : at + 8, :] = powers(decay * decay, pair, (1, 2, 4, 8)) * both
    carry_ref[...] = bands_summed(weigh_ref[...]).reshape(FIELDS, LONS, 8, 128)


def chain_local(both, c1, decay, pair):
    value = scan_pairs(both, decay * decay, pair)
    return value, c1 + decay * jnp.where(pair < 15, later(value, 1), 0.0)


def scan_kernel(pairs_ref, decay_ref, first_ref, second_ref):
    pair = iota(1) // 8
    for f in range(FIELDS):
        for col in range(LONS):
            first_ref[f, col], second_ref[f, col] = chain_local(
                pairs_ref[0, f, col], pairs_ref[1, f, col], decay_ref[f, col], pair
            )


def powers(square, exponent, bits=(1, 2, 4, 8, 16)):
    power = jnp.where((exponent & 1) != 0, square, 1.0)
    for bit in bits[1:]:
        square = square * square
        power = power * jnp.where((exponent & bit) != 0, square, 1.0)
    return power


def open_kernel(
    core_ref,
    mine_ref,
    other_ref,
    zero_ref,
    above_ref,
    decay_ref,
    power_ref,
    turn_ref,
    terms_ref,
    weigh_ref,
    carry_ref,
):
    low = core_ref[0] == 0
    lane = iota(1)
    pair = lane // 8
    even = (pair & 1) == 0

    def turned(half_ref, s):
        turn_ref[pl.ds(0, 64, stride=2), :] = jnp.where(low, half_ref[0], half_ref[1])
        turn_ref[pl.ds(1, 64, stride=2), :] = jnp.where(low, half_ref[1], half_ref[0])
        return turn_ref[...].T

    for s in range(4):
        early, late = (
            [ref[pl.ds(at + s, 64, stride=4), :] for ref in (mine_ref, other_ref)]
            for at in (0, 256)
        )
        here = turned([jnp.where(low, a, b) for a, b in zip(early, late)], s)
        behind = turned(late, s)
        for half in range(2):
            at = 64 * half
            col = s + 4 * half
            mixed = here[at + 48 : at + 56, :]
            decays = (
                jnp.where(even, mixed, pltpu.roll(mixed, 8, 1)),
                here[at + 56 : at + 64, :],
                jnp.where(even, pltpu.roll(mixed, 120, 1), mixed),
            )
            for f in range(FIELDS):
                decay = decays[f]
                decay_ref[f, col] = decay
                for j in range(2):
                    to = at + 24 * j + 8 * f
                    terms_ref[0, j, f, col] = here[to : to + 8, :]
                    terms_ref[1, j, f, col] = behind[to : to + 8, :]
                square = decay * decay
                power_ref[0, f, col] = powers(square, 16 - pair)
                power_ref[1, f, col] = decay * powers(square, 15 - pair, (1, 2, 4, 8))
    chain_first(
        lambda f, col: (terms_ref[1, 0, f, col], terms_ref[1, 1, f, col]),
        decay_ref,
        None,
        carry_ref,
        weigh_ref,
    )
    for f in range(FIELDS):
        for col in range(LONS):
            decay = decay_ref[f, col]
            c0, c1 = terms_ref[0, 0, f, col], terms_ref[0, 1, f, col]
            carry = jnp.where(low, carry_ref[f, col], 0.0)
            c1 = c1 + jnp.where(pair == 15, decay * carry, 0.0)
            value, second = chain_local(c0 + decay * c1, c1, decay, pair)
            zero_ref[f, col] = value
            above_ref[0, f, col] = second
            above_ref[1, f, col] = jnp.where(pair < 15, later(value, 1), carry)


def close_kernel(core_ref, first_ref, second_ref, carry_ref, power_ref, zero_ref, above_ref):
    low = core_ref[0] == 0
    pair = iota(1) // 8
    for f in range(FIELDS):
        for col in range(LONS):
            carry = jnp.where(low, carry_ref[f, col], 0.0)
            value = first_ref[f, col] + power_ref[0, f, col] * carry
            zero_ref[f, col] = value
            above_ref[0, f, col] = second_ref[f, col] + power_ref[1, f, col] * carry
            above_ref[1, f, col] = jnp.where(pair < 15, later(value, 1), carry)


def fine_kernel(
    odd_ref, own_ref, one_ref, two_ref, decay_ref, pairs_ref, carry_ref, state_ref, weigh_ref
):
    odd = odd_ref[0] == 1
    lane = iota(1)
    band = lane % 8
    width = 3 * LONS

    def slot(j, f, col):
        return 24 * ((j * FIELDS + f) * width + col)

    def put(j, f, col, value):
        at = slot(j, f, col) + 8
        state_ref[at : at + 8, :] = value

    def here(j, f, col):
        at = slot(j, f, col) + 8
        return state_ref[at : at + 8, :]

    def rows(j, f, col):
        at = slot(j, f, col) + 8
        return state_ref[at + 1 : at + 9, :], state_ref[at - 1 : at + 7, :]

    def edges(j, f, low, high):
        for col in range(low, high, 8):
            at = slot(j, f, min(col, width - 8))
            first = pltpu.roll(state_ref[pl.ds(at + 8, 8, stride=24), :], 127, 1)
            last = pltpu.roll(state_ref[pl.ds(at + 15, 8, stride=24), :], 1, 1)
            state_ref[pl.ds(at + 16, 8, stride=24), :] = jnp.where(band < 7, first, 0.0)
            state_ref[pl.ds(at + 7, 8, stride=24), :] = jnp.where(band > 0, last, 0.0)

    for j in range(2):
        for f in range(FIELDS):
            for at in range(LONS):
                one, two = one_ref[j, f, at], two_ref[j, f, at]
                put(j, f, at, jnp.where(odd, one, two))
                put(j, f, LONS + at, own_ref[j, f, at])
                put(j, f, 2 * LONS + at, jnp.where(odd, two, one))
            edges(j, f, 0, width)

    keep = 1.0 / diffusion - 4.0
    wave = 0.5 * wave_coef / diffusion
    wave_new = 0.5 * wave_coef
    turn = coriolis / diffusion
    unit = diffusion**STEPS
    result = {}
    for step in range(STEPS):
        low, high = 2 * step + 1, width - 2 * step - 1
        for j in range(2):
            p = {col: here(j, 0, col) for col in (low - 1, low)}
            q = {col: here(j, 1, col) for col in (low - 1, low)}
            for col in range(low, high):
                p[col + 1], q[col + 1] = here(j, 0, col + 1), here(j, 1, col + 1)
                p_next, p_last = rows(j, 0, col)
                r_next, r_last = rows(j, 2, col)
                p1 = ((keep * p[col] + (p[col - 1] + p[col + 1])) + (p_next + p_last)) + wave * (
                    (q[col + 1] - q[col - 1]) + (r_next - r_last)
                )
                put(j, 0, col, p1)
            edges(j, 0, low, high)
        low, high = low + 1, high - 1
        for j in range(2):
            p, q, r = (
                {col: here(j, f, col) for col in (low - 1, low)} for f in range(FIELDS)
            )
            for col in range(low, high):
                p[col + 1], q[col + 1], r[col + 1] = (here(j, f, col + 1) for f in range(FIELDS))
                p_next, p_last = rows(j, 0, col)
                q_next, q_last = rows(j, 1, col)
                r_next, r_last = rows(j, 2, col)
                q1 = (
                    (keep * q[col] + (q[col - 1] + q[col + 1])) + (q_next + q_last)
                ) + (wave_new * (p[col + 1] - p[col - 1]) + turn * r[col])
                r1 = (
                    (keep * r[col] + (r[col - 1] + r[col + 1])) + (r_next + r_last)
                ) + (wave_new * (p_next - p_last) - turn * q[col])
                if step < STEPS - 1:
                    put(j, 1, col, q1)
                    put(j, 2, col, r1)
                else:
                    for f, value in enumerate((p[col], q1, r1)):
                        result[j, f, col - LONS] = value
            if step < STEPS - 1:
                edges(j, 1, low, high)
                edges(j, 2, low, high)

    def terms(f, col):
        return [unit * result[j, f, col] - decay_ref[f, col] * own_ref[j, f, col] for j in range(2)]

    chain_first(terms, decay_ref, pairs_ref, carry_ref, weigh_ref)


def finish_kernel(core_ref, *refs):
    zeros = refs[0:3]
    aboves = refs[3:6]
    first_ref, second_ref, carry_ref, power_ref, misfit_ref = refs[6:11]
    mine_ref, other_ref, turn_ref, back_ref = refs[11:]
    low = core_ref[0] == 0
    pair = iota(1) // 8
    subwindow = (2 * (pair + jnp.where(low, 0, 16))).astype(jnp.float32)
    emphasis = [1.0 + 2.0 * (subwindow + j) / 63.0 for j in range(2)]
    sums = [jnp.zeros((8, 128), jnp.float32) for _ in range(2 * ITERS)]
    result = {}
    for f in range(FIELDS):
        for col in range(LONS):
            carry = jnp.where(low, carry_ref[f, col], 0.0)
            last = (
                first_ref[f, col] + power_ref[0, f, col] * carry,
                second_ref[f, col] + power_ref[1, f, col] * carry,
            )
            for j in range(2):
                so_far = zeros[0][f, col] if j == 0 else aboves[0][0, f, col]
                for n in range(ITERS):
                    if n == ITERS - 1:
                        change = last[j]
                    else:
                        change = zeros[n + 1][f, col] if j == 0 else aboves[n + 1][0, f, col]
                    so_far = so_far + change
                    sums[n] = sums[n] + emphasis[j] * (change * change)
                    sums[ITERS + n] = sums[ITERS + n] + emphasis[j] * (so_far * so_far)
                result[j, f, col] = so_far
    row = iota(0)
    parts = jnp.zeros((8, 128), jnp.float32)
    for at, part in enumerate(sums[:ITERS] + [misfit_ref[...]] + sums[ITERS:]):
        parts = jnp.where(row == at, jnp.sum(part, axis=0, keepdims=True), parts)
    ones = jnp.ones((128, 128), jnp.float32)
    totals = jnp.dot(parts, ones, precision=lax.Precision.HIGHEST)
    turn_ref[48:56, :] = totals
    for s in range(4):
        for half in range(2):
            at = 64 * half
            for j in range(2):
                for f in range(FIELDS):
                    to = at + 24 * j + 8 * f
                    turn_ref[to : to + 8, :] = result[j, f, s + 4 * half]
        back_ref[...] = turn_ref[...].T
        evens = back_ref[pl.ds(0, 64, stride=2), :]
        odds = back_ref[pl.ds(1, 64, stride=2), :]
        mine_ref[pl.ds(s, 64, stride=4), :] = jnp.where(low, evens, odds)
        other_ref[pl.ds(s, 64, stride=4), :] = jnp.where(low, odds, evens)


def join_kernel(core_ref, mine_ref, got_ref, out_ref):
    low = core_ref[0] == 0
    lane = lax.broadcasted_iota(jnp.int32, (256, 128), 1)
    counted = (lane & 120) == 48
    mine, got = mine_ref[...], got_ref[...]
    total = mine + got
    out_ref[0:256, :] = jnp.where(counted, total, jnp.where(low, mine, got))
    out_ref[256:512, :] = jnp.where(counted, total, jnp.where(low, got, mine))


def unpack_kernel(in_ref, out_ref, misfit_ref, changes_ref, rows_ref):
    sums = [in_ref[8 * v : 8 * v + 8, :] for v in range(64)]
    while len(sums) > 1:
        sums = [a + b for a, b in zip(sums[::2], sums[1::2])]
    total = pltpu.roll(sums[0] + pltpu.roll(sums[0], 4, 0), 80, 1)
    misfit_ref[...] = total[0:1, 3:4]
    changes_ref[...] = (total / (pltpu.roll(total, 124, 1) + epsilon))[0:1, 0:ITERS]
    second = (lax.broadcasted_iota(jnp.int32, (128, 128), 0) & 7) >= 4
    for b in range(8):
        for i in range(16):
            at = 4 * chip_of(16 * b + i)
            piece = in_ref[at : at + 4, :]
            rows_ref[8 * i : 8 * i + 4, :] = piece
            rows_ref[8 * i + 4 : 8 * i + 8, :] = piece
        block = rows_ref[...]
        turned = jnp.where(second, pltpu.roll(block, 64, 1), block).T
        for j in range(2):
            for f in range(FIELDS):
                at = 24 * j + 8 * f
                out_ref[j, f, :, 128 * b : 128 * b + 128] = turned[at : at + 8, :]


def per_device(departure, obs_weight, obs_block, coarse_decay):
    z, y, x, core = (lax.axis_index(name) for name in ("z", "y", "x", "c"))
    core_arg = core.astype(jnp.int32).reshape(1)
    tile_odd = ((x + y + z + core) % 2).astype(jnp.int32).reshape(1)
    place = (z * NY + y).astype(jnp.int32).reshape(1)

    position = ((z * NY + y) * 2 + jnp.arange(2)).astype(jnp.float32)
    strength = (1.0 + 2.0 * position / 63.0)[:, None] * obs_weight
    misfit_part = 0.5 * jnp.sum(
        strength[:, :, None, None] * departure * departure, axis=(0, 1, 2)
    ).reshape(8, 128)

    sent = call(
        pack_kernel,
        shape(512, 128),
        (place,),
        far=(departure.transpose(0, 2, 1, 3), obs_weight, obs_block, coarse_decay),
        scratch=[
            pltpu.VMEM((2, FIELDS, 16, 1024), jnp.float32),
            pltpu.VMEM((2, 16), jnp.float32),
            pltpu.VMEM((2, 16), jnp.int32),
            pltpu.VMEM((FIELDS, 8, 1024), jnp.float32),
            pltpu.VMEM((512, 128), jnp.float32),
            pltpu.SemaphoreType.DMA((9,)),
        ],
    )
    got = lax.all_to_all(sent.reshape(CHIPS, 4, 128), ZYX, 0, 0).reshape(512, 128)
    other = lax.ppermute(got, "c", SIBLING)

    field = shape(FIELDS, LONS, 8, 128)
    both = shape(2, FIELDS, LONS, 8, 128)
    square = pltpu.VMEM((128, 128), jnp.float32)
    weigh = pltpu.VMEM((FIELDS * LONS * 8, 128), jnp.float32)
    zero, above, decay, power = call(
        open_kernel,
        (field, both, field, both),
        (core_arg,),
        got,
        other,
        scratch=[
            square,
            pltpu.VMEM((2, 2, FIELDS, LONS, 8, 128), jnp.float32),
            weigh,
            pltpu.VMEM((FIELDS, LONS, 8, 128), jnp.float32),
        ],
    )
    zeros, aboves = [], []
    for iteration in range(ITERS):
        if iteration > 0:
            zero, above = call(
                close_kernel, (field, both), (core_arg,), first, second, carry, power
            )
        zeros.append(zero)
        aboves.append(above)
        side_one = lax.ppermute(above, ALL, swap_pairs(0))
        side_two = lax.ppermute(above, ALL, swap_pairs(1))
        pairs, carry = call(
            fine_kernel,
            (both, field),
            (tile_odd,),
            above,
            side_one,
            side_two,
            decay,
            scratch=[pltpu.VMEM((2 * FIELDS * 3 * LONS * 24, 128), jnp.float32), weigh],
        )
        carry = lax.ppermute(carry, "c", SIBLING)
        first, second = call(scan_kernel, (field, field), (), pairs, decay)
    mine, away = call(
        finish_kernel,
        (shape(256, 128), shape(256, 128)),
        (core_arg,),
        *zeros,
        *aboves,
        first,
        second,
        carry,
        power,
        misfit_part,
        scratch=[square, square],
    )
    other = lax.ppermute(away, "c", SIBLING)
    back = call(join_kernel, shape(512, 128), (core_arg,), mine, other)
    home = lax.all_to_all(back.reshape(CHIPS, 4, 128), ZYX, 0, 0).reshape(512, 128)
    adjoint, misfit, changes = call(
        unpack_kernel,
        (
            jax.ShapeDtypeStruct((2, FIELDS, 8, 1024), jnp.float32),
            jax.ShapeDtypeStruct((1, 1), jnp.float32),
            jax.ShapeDtypeStruct((1, ITERS), jnp.float32),
        ),
        (),
        home,
        scratch=[square],
    )
    return adjoint, misfit.reshape(()), changes.reshape(ITERS)


def solution(mesh):
    split = Mesh(mesh.devices.reshape(NZ, NY, NX, 2), ("z", "y", "x", "c"))
    return jax.shard_map(
        per_device,
        mesh=split,
        in_specs=(P(TM, GRID, None, None), P(TM, GRID), P(TM, GRID), P(None, GRID, None)),
        out_specs=(P(TM, None, GRID, None), P(), P()),
        check_vma=False,
    )
```

```python
import functools

import jax
import jax.numpy as jnp
from jax import lax
from jax.experimental import pallas as pl
from jax.experimental.pallas import tpu as pltpu
from jax.sharding import Mesh
from jax.sharding import PartitionSpec as P

STEPS = 4
ITERS = 3
NZ, NY, NX = 8, 4, 4
CHIPS = NZ * NY * NX
LONS = 8
FIELDS = 3
TM = ("z", "y")
GRID = ("x", "c")
ZYX = ("z", "y", "x")
ALL = ("z", "y", "x", "c")

wave_coef = 0.6
diffusion = 0.05
coriolis = 0.1
epsilon = 1e-06


def chip_of(tile):
    z, place = divmod(tile, NY * NX)
    if z % 2:
        place = NY * NX - 1 - place
    y, x = divmod(place, NX)
    if y % 2:
        x = NX - 1 - x
    return (z * NY + y) * NX + x


def swap_pairs(first):
    pairs = []
    for tile in range(CHIPS):
        core = (tile + first) % 2
        a, b = 2 * chip_of(tile) + core, 2 * chip_of((tile + 1) % CHIPS) + core
        pairs += [(a, b), (b, a)]
    return pairs


SIBLING = [(0, 1), (1, 0)]


def shape(*dims):
    return pltpu.VMEM(dims, jnp.float32)


def near(value):
    return pltpu.with_memory_space_constraint(value, pltpu.VMEM)


def call(kernel, outs, scalars, *operands, far=(), scratch=()):
    vmem = pl.BlockSpec(memory_space=pltpu.VMEM)
    hbm = pl.BlockSpec(memory_space=pl.ANY)
    smem = pl.BlockSpec(memory_space=pltpu.SMEM)
    outs = outs if isinstance(outs, tuple) else (outs,)
    results = pl.pallas_call(
        kernel,
        out_shape=outs,
        in_specs=[smem] * len(scalars) + [hbm] * len(far) + [vmem] * len(operands),
        out_specs=[vmem] * len(outs),
        scratch_shapes=list(scratch),
    )(*scalars, *far, *map(near, operands))
    return results if len(outs) > 1 else results[0]


def iota(dim):
    return lax.broadcasted_iota(jnp.int32, (8, 128), dim)


def split(values):
    high = values.astype(jnp.bfloat16)
    return high, (values - high.astype(jnp.float32)).astype(jnp.bfloat16)


def pack_kernel(
    place_ref,
    departure_ref,
    weight_ref,
    block_ref,
    decay_ref,
    out_ref,
    values_ref,
    weights_ref,
    blocks_ref,
    decays_ref,
    rows_ref,
    sems,
):
    copies = [
        pltpu.make_async_copy(weight_ref, weights_ref, sems.at[0]),
        pltpu.make_async_copy(block_ref, blocks_ref, sems.at[1]),
        pltpu.make_async_copy(departure_ref, values_ref, sems.at[2]),
        pltpu.make_async_copy(decay_ref, decays_ref, sems.at[3]),
    ]
    for copy in copies:
        copy.start()
    for copy in copies:
        copy.wait()
    block = lax.broadcasted_iota(jnp.int32, (8, 16), 0)
    for j in range(2):
        emphasis = 1.0 + 2.0 * (place_ref[0] * 2 + j).astype(jnp.float32) / 63.0
        choose = jnp.where(
            blocks_ref[j : j + 1, :] == block, emphasis * weights_ref[j : j + 1, :], 0.0
        )
        choose_high, choose_low = split(choose)
        choose_both = jnp.concatenate([choose_high, choose_low], axis=0)
        for f in range(FIELDS):
            values_high, values_low = split(values_ref[j, f])
            main = jnp.dot(choose_both, values_high, preferred_element_type=jnp.float32)
            rest = jnp.dot(choose_high, values_low, preferred_element_type=jnp.float32)
            tiles = main[0:8] + (main[8:16] + rest)
            for r in range(8):
                rows_ref[pl.ds(24 * j + 8 * f + r, 8, stride=64), :] = tiles[
                    :, 128 * r : 128 * r + 128
                ]
    odd = (place_ref[0] & 1) == 1
    for b in range(8):
        span = slice(128 * b, 128 * b + 128)
        rows_ref[64 * b + 48 : 64 * b + 56, :] = jnp.where(
            odd, decays_ref[2, :, span], decays_ref[0, :, span]
        )
        rows_ref[64 * b + 56 : 64 * b + 64, :] = decays_ref[1, :, span]
    for b in range(8):
        block = rows_ref[64 * b : 64 * b + 64, :]
        both = jnp.concatenate([block, pltpu.roll(block, 124, 1)], axis=0)
        turned = both.T
        for i in range(16):
            to = 4 * chip_of(16 * b + i)
            out_ref[to : to + 4, :] = turned[8 * i : 8 * i + 4, :]


def later(value, groups):
    return pltpu.roll(value, 128 - 8 * groups, value.ndim - 1)


def scan_pairs(u, square, pair):
    for groups in (1, 4):
        factor = square
        total = u
        for times in (1, 2, 3):
            back = times * groups
            total = total + jnp.where(pair < 16 - back, factor, 0.0) * later(u, back)
            factor = factor * square
        u, square = total, factor
    return u


def bands_summed(values):
    source = lax.broadcasted_iota(jnp.int32, (128, 128), 0)
    target = lax.broadcasted_iota(jnp.int32, (128, 128), 1)
    same = (source % 8 == target % 8).astype(jnp.float32)
    return jnp.dot(
        values, same, precision=lax.Precision.HIGHEST, preferred_element_type=jnp.float32
    )


def chain_first(terms_of, decay_ref, pairs_ref, carry_ref, weigh_ref):
    pair = iota(1) // 8
    for f in range(FIELDS):
        for col in range(LONS):
            decay = decay_ref[f, col]
            c0, c1 = terms_of(f, col)
            both = c0 + decay * c1
            if pairs_ref is not None:
                pairs_ref[0, f, col] = both
                pairs_ref[1, f, col] = c1
            at = 8 * (LONS * f + col)
            weigh_ref[at : at + 8, :] = powers(decay * decay, pair, (1, 2, 4, 8)) * both
    carry_ref[...] = bands_summed(weigh_ref[...]).reshape(FIELDS, LONS, 8, 128)


def chain_local(both, c1, decay, pair):
    value = scan_pairs(both, decay * decay, pair)
    return value, c1 + decay * jnp.where(pair < 15, later(value, 1), 0.0)


def scan_kernel(pairs_ref, decay_ref, first_ref, second_ref):
    pair = iota(1) // 8
    for f in range(FIELDS):
        for col in range(LONS):
            first_ref[f, col], second_ref[f, col] = chain_local(
                pairs_ref[0, f, col], pairs_ref[1, f, col], decay_ref[f, col], pair
            )


def powers(square, exponent, bits=(1, 2, 4, 8, 16)):
    power = jnp.where((exponent & 1) != 0, square, 1.0)
    for bit in bits[1:]:
        square = square * square
        power = power * jnp.where((exponent & bit) != 0, square, 1.0)
    return power


def open_kernel(
    core_ref,
    mine_ref,
    other_ref,
    zero_ref,
    above_ref,
    decay_ref,
    power_ref,
    turn_ref,
    terms_ref,
    weigh_ref,
    carry_ref,
):
    low = core_ref[0] == 0
    lane = iota(1)
    pair = lane // 8
    even = (pair & 1) == 0

    def turned(half_ref, s):
        turn_ref[pl.ds(0, 64, stride=2), :] = jnp.where(low, half_ref[0], half_ref[1])
        turn_ref[pl.ds(1, 64, stride=2), :] = jnp.where(low, half_ref[1], half_ref[0])
        return turn_ref[...].T

    for s in range(4):
        early, late = (
            [ref[pl.ds(at + s, 64, stride=4), :] for ref in (mine_ref, other_ref)]
            for at in (0, 256)
        )
        here = turned([jnp.where(low, a, b) for a, b in zip(early, late)], s)
        behind = turned(late, s)
        for half in range(2):
            at = 64 * half
            col = s + 4 * half
            mixed = here[at + 48 : at + 56, :]
            decays = (
                jnp.where(even, mixed, pltpu.roll(mixed, 8, 1)),
                here[at + 56 : at + 64, :],
                jnp.where(even, pltpu.roll(mixed, 120, 1), mixed),
            )
            for f in range(FIELDS):
                decay = decays[f]
                decay_ref[f, col] = decay
                for j in range(2):
                    to = at + 24 * j + 8 * f
                    terms_ref[0, j, f, col] = here[to : to + 8, :]
                    terms_ref[1, j, f, col] = behind[to : to + 8, :]
                square = decay * decay
                power_ref[0, f, col] = powers(square, 16 - pair)
                power_ref[1, f, col] = decay * powers(square, 15 - pair, (1, 2, 4, 8))
    chain_first(
        lambda f, col: (terms_ref[1, 0, f, col], terms_ref[1, 1, f, col]),
        decay_ref,
        None,
        carry_ref,
        weigh_ref,
    )
    for f in range(FIELDS):
        for col in range(LONS):
            decay = decay_ref[f, col]
            c0, c1 = terms_ref[0, 0, f, col], terms_ref[0, 1, f, col]
            carry = jnp.where(low, carry_ref[f, col], 0.0)
            c1 = c1 + jnp.where(pair == 15, decay * carry, 0.0)
            value, second = chain_local(c0 + decay * c1, c1, decay, pair)
            zero_ref[f, col] = value
            above_ref[0, f, col] = second
            above_ref[1, f, col] = jnp.where(pair < 15, later(value, 1), carry)


def close_kernel(core_ref, first_ref, second_ref, carry_ref, power_ref, zero_ref, above_ref):
    low = core_ref[0] == 0
    pair = iota(1) // 8
    for f in range(FIELDS):
        for col in range(LONS):
            carry = jnp.where(low, carry_ref[f, col], 0.0)
            value = first_ref[f, col] + power_ref[0, f, col] * carry
            zero_ref[f, col] = value
            above_ref[0, f, col] = second_ref[f, col] + power_ref[1, f, col] * carry
            above_ref[1, f, col] = jnp.where(pair < 15, later(value, 1), carry)


def fine_kernel(
    odd_ref, own_ref, one_ref, two_ref, decay_ref, pairs_ref, carry_ref, state_ref, weigh_ref
):
    odd = odd_ref[0] == 1
    lane = iota(1)
    band = lane % 8
    width = 3 * LONS

    def slot(j, f, col):
        return 24 * ((j * FIELDS + f) * width + col)

    def put(j, f, col, value):
        at = slot(j, f, col) + 8
        state_ref[at : at + 8, :] = value

    def here(j, f, col):
        at = slot(j, f, col) + 8
        return state_ref[at : at + 8, :]

    def rows(j, f, col):
        at = slot(j, f, col) + 8
        return state_ref[at + 1 : at + 9, :], state_ref[at - 1 : at + 7, :]

    def edges(j, f, low, high):
        for col in range(low, high, 8):
            at = slot(j, f, min(col, width - 8))
            first = pltpu.roll(state_ref[pl.ds(at + 8, 8, stride=24), :], 127, 1)
            last = pltpu.roll(state_ref[pl.ds(at + 15, 8, stride=24), :], 1, 1)
            state_ref[pl.ds(at + 16, 8, stride=24), :] = jnp.where(band < 7, first, 0.0)
            state_ref[pl.ds(at + 7, 8, stride=24), :] = jnp.where(band > 0, last, 0.0)

    for j in range(2):
        for f in range(FIELDS):
            for at in range(LONS):
                one, two = one_ref[j, f, at], two_ref[j, f, at]
                put(j, f, at, jnp.where(odd, one, two))
                put(j, f, LONS + at, own_ref[j, f, at])
                put(j, f, 2 * LONS + at, jnp.where(odd, two, one))
            edges(j, f, 0, width)

    keep = 1.0 / diffusion - 4.0
    wave = 0.5 * wave_coef / diffusion
    wave_new = 0.5 * wave_coef
    turn = coriolis / diffusion
    unit = diffusion**STEPS
    result = {}
    for step in range(STEPS):
        low, high = 2 * step + 1, width - 2 * step - 1
        for j in range(2):
            p = {col: here(j, 0, col) for col in (low - 1, low)}
            q = {col: here(j, 1, col) for col in (low - 1, low)}
            for col in range(low, high):
                p[col + 1], q[col + 1] = here(j, 0, col + 1), here(j, 1, col + 1)
                p_next, p_last = rows(j, 0, col)
                r_next, r_last = rows(j, 2, col)
                p1 = ((keep * p[col] + (p[col - 1] + p[col + 1])) + (p_next + p_last)) + wave * (
                    (q[col + 1] - q[col - 1]) + (r_next - r_last)
                )
                put(j, 0, col, p1)
            edges(j, 0, low, high)
        low, high = low + 1, high - 1
        for j in range(2):
            p, q, r = (
                {col: here(j, f, col) for col in (low - 1, low)} for f in range(FIELDS)
            )
            for col in range(low, high):
                p[col + 1], q[col + 1], r[col + 1] = (here(j, f, col + 1) for f in range(FIELDS))
                p_next, p_last = rows(j, 0, col)
                q_next, q_last = rows(j, 1, col)
                r_next, r_last = rows(j, 2, col)
                q1 = (
                    (keep * q[col] + (q[col - 1] + q[col + 1])) + (q_next + q_last)
                ) + (wave_new * (p[col + 1] - p[col - 1]) + turn * r[col])
                r1 = (
                    (keep * r[col] + (r[col - 1] + r[col + 1])) + (r_next + r_last)
                ) + (wave_new * (p_next - p_last) - turn * q[col])
                if step < STEPS - 1:
                    put(j, 1, col, q1)
                    put(j, 2, col, r1)
                else:
                    for f, value in enumerate((p[col], q1, r1)):
                        result[j, f, col - LONS] = value
            if step < STEPS - 1:
                edges(j, 1, low, high)
                edges(j, 2, low, high)

    def terms(f, col):
        return [unit * result[j, f, col] - decay_ref[f, col] * own_ref[j, f, col] for j in range(2)]

    chain_first(terms, decay_ref, pairs_ref, carry_ref, weigh_ref)


def finish_kernel(core_ref, *refs):
    zeros = refs[0:3]
    aboves = refs[3:6]
    first_ref, second_ref, carry_ref, power_ref, misfit_ref = refs[6:11]
    mine_ref, other_ref, turn_ref, back_ref = refs[11:]
    low = core_ref[0] == 0
    pair = iota(1) // 8
    subwindow = (2 * (pair + jnp.where(low, 0, 16))).astype(jnp.float32)
    emphasis = [1.0 + 2.0 * (subwindow + j) / 63.0 for j in range(2)]
    sums = [jnp.zeros((8, 128), jnp.float32) for _ in range(2 * ITERS)]
    result = {}
    for f in range(FIELDS):
        for col in range(LONS):
            carry = jnp.where(low, carry_ref[f, col], 0.0)
            last = (
                first_ref[f, col] + power_ref[0, f, col] * carry,
                second_ref[f, col] + power_ref[1, f, col] * carry,
            )
            for j in range(2):
                so_far = zeros[0][f, col] if j == 0 else aboves[0][0, f, col]
                for n in range(ITERS):
                    if n == ITERS - 1:
                        change = last[j]
                    else:
                        change = zeros[n + 1][f, col] if j == 0 else aboves[n + 1][0, f, col]
                    so_far = so_far + change
                    sums[n] = sums[n] + emphasis[j] * (change * change)
                    sums[ITERS + n] = sums[ITERS + n] + emphasis[j] * (so_far * so_far)
                result[j, f, col] = so_far
    row = iota(0)
    parts = jnp.zeros((8, 128), jnp.float32)
    for at, part in enumerate(sums[:ITERS] + [misfit_ref[...]] + sums[ITERS:]):
        parts = jnp.where(row == at, jnp.sum(part, axis=0, keepdims=True), parts)
    ones = jnp.ones((128, 128), jnp.float32)
    totals = jnp.dot(parts, ones, precision=lax.Precision.HIGHEST)
    turn_ref[48:56, :] = totals
    for s in range(4):
        for half in range(2):
            at = 64 * half
            for j in range(2):
                for f in range(FIELDS):
                    to = at + 24 * j + 8 * f
                    turn_ref[to : to + 8, :] = result[j, f, s + 4 * half]
        back_ref[...] = turn_ref[...].T
        evens = back_ref[pl.ds(0, 64, stride=2), :]
        odds = back_ref[pl.ds(1, 64, stride=2), :]
        mine_ref[pl.ds(s, 64, stride=4), :] = jnp.where(low, evens, odds)
        other_ref[pl.ds(s, 64, stride=4), :] = jnp.where(low, odds, evens)


def join_kernel(core_ref, mine_ref, got_ref, out_ref):
    low = core_ref[0] == 0
    lane = lax.broadcasted_iota(jnp.int32, (256, 128), 1)
    counted = (lane & 120) == 48
    mine, got = mine_ref[...], got_ref[...]
    total = mine + got
    out_ref[0:256, :] = jnp.where(counted, total, jnp.where(low, mine, got))
    out_ref[256:512, :] = jnp.where(counted, total, jnp.where(low, got, mine))


def unpack_kernel(in_ref, out_ref, misfit_ref, changes_ref, rows_ref):
    sums = [in_ref[8 * v : 8 * v + 8, :] for v in range(64)]
    while len(sums) > 1:
        sums = [a + b for a, b in zip(sums[::2], sums[1::2])]
    total = pltpu.roll(sums[0] + pltpu.roll(sums[0], 4, 0), 80, 1)
    misfit_ref[...] = total[0:1, 3:4]
    changes_ref[...] = (total / (pltpu.roll(total, 124, 1) + epsilon))[0:1, 0:ITERS]
    second = (lax.broadcasted_iota(jnp.int32, (128, 128), 0) & 7) >= 4
    for b in range(8):
        for i in range(16):
            at = 4 * chip_of(16 * b + i)
            piece = in_ref[at : at + 4, :]
            rows_ref[8 * i : 8 * i + 4, :] = piece
            rows_ref[8 * i + 4 : 8 * i + 8, :] = piece
        block = rows_ref[...]
        turned = jnp.where(second, pltpu.roll(block, 64, 1), block).T
        for j in range(2):
            for f in range(FIELDS):
                at = 24 * j + 8 * f
                out_ref[j, f, :, 128 * b : 128 * b + 128] = turned[at : at + 8, :]


def per_device(departure, obs_weight, obs_block, coarse_decay):
    z, y, x, core = (lax.axis_index(name) for name in ("z", "y", "x", "c"))
    core_arg = core.astype(jnp.int32).reshape(1)
    tile_odd = ((x + y + z + core) % 2).astype(jnp.int32).reshape(1)
    place = (z * NY + y).astype(jnp.int32).reshape(1)

    position = ((z * NY + y) * 2 + jnp.arange(2)).astype(jnp.float32)
    strength = (1.0 + 2.0 * position / 63.0)[:, None] * obs_weight
    misfit_part = 0.5 * jnp.sum(
        strength[:, :, None, None] * departure * departure, axis=(0, 1, 2)
    ).reshape(8, 128)

    sent = call(
        pack_kernel,
        shape(512, 128),
        (place,),
        far=(departure.transpose(0, 2, 1, 3), obs_weight, obs_block, coarse_decay),
        scratch=[
            pltpu.VMEM((2, FIELDS, 16, 1024), jnp.float32),
            pltpu.VMEM((2, 16), jnp.float32),
            pltpu.VMEM((2, 16), jnp.int32),
            pltpu.VMEM((FIELDS, 8, 1024), jnp.float32),
            pltpu.VMEM((512, 128), jnp.float32),
            pltpu.SemaphoreType.DMA((4,)),
        ],
    )
    got = lax.all_to_all(sent.reshape(CHIPS, 4, 128), ZYX, 0, 0).reshape(512, 128)
    other = lax.ppermute(got, "c", SIBLING)

    field = shape(FIELDS, LONS, 8, 128)
    both = shape(2, FIELDS, LONS, 8, 128)
    square = pltpu.VMEM((128, 128), jnp.float32)
    weigh = pltpu.VMEM((FIELDS * LONS * 8, 128), jnp.float32)
    zero, above, decay, power = call(
        open_kernel,
        (field, both, field, both),
        (core_arg,),
        got,
        other,
        scratch=[
            square,
            pltpu.VMEM((2, 2, FIELDS, LONS, 8, 128), jnp.float32),
            weigh,
            pltpu.VMEM((FIELDS, LONS, 8, 128), jnp.float32),
        ],
    )
    zeros, aboves = [], []
    for iteration in range(ITERS):
        if iteration > 0:
            zero, above = call(
                close_kernel, (field, both), (core_arg,), first, second, carry, power
            )
        zeros.append(zero)
        aboves.append(above)
        side_one = lax.ppermute(above, ALL, swap_pairs(0))
        side_two = lax.ppermute(above, ALL, swap_pairs(1))
        pairs, carry = call(
            fine_kernel,
            (both, field),
            (tile_odd,),
            above,
            side_one,
            side_two,
            decay,
            scratch=[pltpu.VMEM((2 * FIELDS * 3 * LONS * 24, 128), jnp.float32), weigh],
        )
        carry = lax.ppermute(carry, "c", SIBLING)
        first, second = call(scan_kernel, (field, field), (), pairs, decay)
    mine, away = call(
        finish_kernel,
        (shape(256, 128), shape(256, 128)),
        (core_arg,),
        *zeros,
        *aboves,
        first,
        second,
        carry,
        power,
        misfit_part,
        scratch=[square, square],
    )
    other = lax.ppermute(away, "c", SIBLING)
    back = call(join_kernel, shape(512, 128), (core_arg,), mine, other)
    home = lax.all_to_all(back.reshape(CHIPS, 4, 128), ZYX, 0, 0).reshape(512, 128)
    adjoint, misfit, changes = call(
        unpack_kernel,
        (
            jax.ShapeDtypeStruct((2, FIELDS, 8, 1024), jnp.float32),
            jax.ShapeDtypeStruct((1, 1), jnp.float32),
            jax.ShapeDtypeStruct((1, ITERS), jnp.float32),
        ),
        (),
        home,
        scratch=[square],
    )
    return adjoint, misfit.reshape(()), changes.reshape(ITERS)


def solution(mesh):
    split = Mesh(mesh.devices.reshape(NZ, NY, NX, 2), ("z", "y", "x", "c"))
    return jax.shard_map(
        per_device,
        mesh=split,
        in_specs=(P(TM, GRID, None, None), P(TM, GRID), P(TM, GRID), P(None, GRID, None)),
        out_specs=(P(TM, None, GRID, None), P(), P()),
        check_vma=False,
    )
```

```python
import functools

import jax
import jax.numpy as jnp
from jax import lax
from jax.experimental import pallas as pl
from jax.experimental.pallas import tpu as pltpu
from jax.sharding import Mesh
from jax.sharding import PartitionSpec as P

STEPS = 4
ITERS = 3
NZ, NY, NX = 8, 4, 4
CHIPS = NZ * NY * NX
LONS = 8
FIELDS = 3
CELLS = 2 * FIELDS * LONS
TM = ("z", "y")
GRID = ("x", "c")
ZYX = ("z", "y", "x")
ALL = ("z", "y", "x", "c")

wave_coef = 0.6
diffusion = 0.05
coriolis = 0.1
epsilon = 1e-06


def chip_of(tile):
    z, place = divmod(tile, NY * NX)
    if z % 2:
        place = NY * NX - 1 - place
    y, x = divmod(place, NX)
    if y % 2:
        x = NX - 1 - x
    return (z * NY + y) * NX + x


def swap_pairs(first):
    pairs = []
    for tile in range(CHIPS):
        core = (tile + first) % 2
        a, b = 2 * chip_of(tile) + core, 2 * chip_of((tile + 1) % CHIPS) + core
        pairs += [(a, b), (b, a)]
    return pairs


SIBLING = [(0, 1), (1, 0)]


def shape(*dims):
    return pltpu.VMEM(dims, jnp.float32)


def near(value):
    return pltpu.with_memory_space_constraint(value, pltpu.VMEM)


def call(kernel, outs, scalars, *operands, far=(), scratch=()):
    vmem = pl.BlockSpec(memory_space=pltpu.VMEM)
    hbm = pl.BlockSpec(memory_space=pl.ANY)
    smem = pl.BlockSpec(memory_space=pltpu.SMEM)
    outs = outs if isinstance(outs, tuple) else (outs,)
    results = pl.pallas_call(
        kernel,
        out_shape=outs,
        in_specs=[smem] * len(scalars) + [hbm] * len(far) + [vmem] * len(operands),
        out_specs=[vmem] * len(outs),
        scratch_shapes=list(scratch),
    )(*scalars, *far, *map(near, operands))
    return results if len(outs) > 1 else results[0]


def iota(dim):
    return lax.broadcasted_iota(jnp.int32, (8, 128), dim)


def split(values):
    high = values.astype(jnp.bfloat16)
    return high, (values - high.astype(jnp.float32)).astype(jnp.bfloat16)


def pack_kernel(
    place_ref,
    departure_ref,
    weight_ref,
    block_ref,
    decay_ref,
    out_ref,
    values_ref,
    weights_ref,
    blocks_ref,
    decays_ref,
    rows_ref,
    sems,
):
    copies = [
        pltpu.make_async_copy(weight_ref, weights_ref, sems.at[0]),
        pltpu.make_async_copy(block_ref, blocks_ref, sems.at[1]),
        pltpu.make_async_copy(departure_ref, values_ref, sems.at[2]),
        pltpu.make_async_copy(decay_ref, decays_ref, sems.at[3]),
    ]
    for copy in copies:
        copy.start()
    for copy in copies:
        copy.wait()
    block = lax.broadcasted_iota(jnp.int32, (8, 16), 0)
    for j in range(2):
        emphasis = 1.0 + 2.0 * (place_ref[0] * 2 + j).astype(jnp.float32) / 63.0
        choose = jnp.where(
            blocks_ref[j : j + 1, :] == block, emphasis * weights_ref[j : j + 1, :], 0.0
        )
        choose_high, choose_low = split(choose)
        choose_both = jnp.concatenate([choose_high, choose_low], axis=0)
        for f in range(FIELDS):
            values_high, values_low = split(values_ref[j, f])
            main = jnp.dot(choose_both, values_high, preferred_element_type=jnp.float32)
            rest = jnp.dot(choose_high, values_low, preferred_element_type=jnp.float32)
            tiles = main[0:8] + (main[8:16] + rest)
            for r in range(8):
                rows_ref[pl.ds(24 * j + 8 * f + r, 8, stride=64), :] = tiles[
                    :, 128 * r : 128 * r + 128
                ]
    odd = (place_ref[0] & 1) == 1
    for b in range(8):
        span = slice(128 * b, 128 * b + 128)
        rows_ref[64 * b + 48 : 64 * b + 56, :] = jnp.where(
            odd, decays_ref[2, :, span], decays_ref[0, :, span]
        )
        rows_ref[64 * b + 56 : 64 * b + 64, :] = decays_ref[1, :, span]
    for b in range(8):
        block = rows_ref[64 * b : 64 * b + 64, :]
        both = jnp.concatenate([block, pltpu.roll(block, 124, 1)], axis=0)
        turned = both.T
        for i in range(16):
            to = 4 * chip_of(16 * b + i)
            out_ref[to : to + 4, :] = turned[8 * i : 8 * i + 4, :]


def later(value, groups):
    return pltpu.roll(value, 128 - 8 * groups, value.ndim - 1)


def scan_pairs(u, square, pair):
    for groups in (1, 4):
        factor = square
        total = u
        for times in (1, 2, 3):
            back = times * groups
            total = total + jnp.where(pair < 16 - back, factor, 0.0) * later(u, back)
            factor = factor * square
        u, square = total, factor
    return u


def bands_summed(values):
    source = lax.broadcasted_iota(jnp.int32, (128, 128), 0)
    target = lax.broadcasted_iota(jnp.int32, (128, 128), 1)
    same = (source % 8 == target % 8).astype(jnp.float32)
    return jnp.dot(
        values, same, precision=lax.Precision.HIGHEST, preferred_element_type=jnp.float32
    )


def chain_first(terms_of, decay_ref, pairs_ref, carry_ref, weigh_ref, both_of=None):
    pair = iota(1) // 8
    for f in range(FIELDS):
        for col in range(LONS):
            decay = decay_ref[f, col]
            if both_of is None:
                c0, c1 = terms_of(f, col)
                both = c0 + decay * c1
            else:
                both = both_of(f, col)
            if pairs_ref is not None:
                pairs_ref[0, f, col] = both
                pairs_ref[1, f, col] = c1
            if carry_ref is not None:
                at = 8 * (LONS * f + col)
                weigh_ref[at : at + 8, :] = powers(decay * decay, pair, (1, 2, 4, 8)) * both
    if carry_ref is not None:
        carry_ref[...] = bands_summed(weigh_ref[...]).reshape(FIELDS, LONS, 8, 128)


def chain_local(both, c1, decay, pair):
    value = scan_pairs(both, decay * decay, pair)
    return value, c1 + decay * jnp.where(pair < 15, later(value, 1), 0.0)


def scan_kernel(pairs_ref, decay_ref, first_ref, second_ref):
    pair = iota(1) // 8
    for f in range(FIELDS):
        for col in range(LONS):
            first_ref[f, col], second_ref[f, col] = chain_local(
                pairs_ref[0, f, col], pairs_ref[1, f, col], decay_ref[f, col], pair
            )


def powers(square, exponent, bits=(1, 2, 4, 8, 16)):
    power = jnp.where((exponent & 1) != 0, square, 1.0)
    for bit in bits[1:]:
        square = square * square
        power = power * jnp.where((exponent & bit) != 0, square, 1.0)
    return power


def open_kernel(
    core_ref,
    mine_ref,
    other_ref,
    zero_ref,
    above_ref,
    decay_ref,
    power_ref,
    turn_ref,
    terms_ref,
    weigh_ref,
    carry_ref,
):
    low = core_ref[0] == 0
    lane = iota(1)
    pair = lane // 8
    even = (pair & 1) == 0

    def turned(half_ref, s):
        turn_ref[pl.ds(0, 64, stride=2), :] = jnp.where(low, half_ref[0], half_ref[1])
        turn_ref[pl.ds(1, 64, stride=2), :] = jnp.where(low, half_ref[1], half_ref[0])
        return turn_ref[...].T

    for s in range(4):
        early, late = (
            [ref[pl.ds(at + s, 64, stride=4), :] for ref in (mine_ref, other_ref)]
            for at in (0, 256)
        )
        here = turned([jnp.where(low, a, b) for a, b in zip(early, late)], s)
        behind = turned(late, s)
        for half in range(2):
            at = 64 * half
            col = s + 4 * half
            mixed = here[at + 48 : at + 56, :]
            decays = (
                jnp.where(even, mixed, pltpu.roll(mixed, 8, 1)),
                here[at + 56 : at + 64, :],
                jnp.where(even, pltpu.roll(mixed, 120, 1), mixed),
            )
            for f in range(FIELDS):
                decay = decays[f]
                decay_ref[f, col] = decay
                for j in range(2):
                    to = at + 24 * j + 8 * f
                    terms_ref[0, j, f, col] = here[to : to + 8, :]
                    terms_ref[1, j, f, col] = behind[to : to + 8, :]
                square = decay * decay
                power_ref[0, f, col] = powers(square, 16 - pair)
                power_ref[1, f, col] = decay * powers(square, 15 - pair, (1, 2, 4, 8))
    chain_first(
        lambda f, col: (terms_ref[1, 0, f, col], terms_ref[1, 1, f, col]),
        decay_ref,
        None,
        carry_ref,
        weigh_ref,
    )
    for f in range(FIELDS):
        for col in range(LONS):
            decay = decay_ref[f, col]
            c0, c1 = terms_ref[0, 0, f, col], terms_ref[0, 1, f, col]
            carry = jnp.where(low, carry_ref[f, col], 0.0)
            c1 = c1 + jnp.where(pair == 15, decay * carry, 0.0)
            value, second = chain_local(c0 + decay * c1, c1, decay, pair)
            zero_ref[f, col] = value
            above_ref[0, f, col] = second
            above_ref[1, f, col] = jnp.where(pair < 15, later(value, 1), carry)


def close_kernel(core_ref, first_ref, second_ref, carry_ref, power_ref, zero_ref, above_ref):
    low = core_ref[0] == 0
    pair = iota(1) // 8
    for f in range(FIELDS):
        for col in range(LONS):
            carry = jnp.where(low, carry_ref[f, col], 0.0)
            value = first_ref[f, col] + power_ref[0, f, col] * carry
            zero_ref[f, col] = value
            above_ref[0, f, col] = second_ref[f, col] + power_ref[1, f, col] * carry
            above_ref[1, f, col] = jnp.where(pair < 15, later(value, 1), carry)


def fine_kernel(
    odd_ref, own_ref, one_ref, two_ref, decay_ref, pairs_ref, *rest
):
    carry_ref, state_ref, weigh_ref = rest if len(rest) == 3 else (None, *rest, None)
    odd = odd_ref[0] == 1
    lane = iota(1)
    band = lane % 8
    width = 3 * LONS

    def slot(j, f, col):
        return 24 * ((j * FIELDS + f) * width + col)

    def put(j, f, col, value):
        at = slot(j, f, col) + 8
        state_ref[at : at + 8, :] = value

    def here(j, f, col):
        at = slot(j, f, col) + 8
        return state_ref[at : at + 8, :]

    def rows(j, f, col):
        at = slot(j, f, col) + 8
        return state_ref[at + 1 : at + 9, :], state_ref[at - 1 : at + 7, :]

    def edges(j, f, low, high):
        for col in range(low, high, 8):
            at = slot(j, f, min(col, width - 8))
            first = pltpu.roll(state_ref[pl.ds(at + 8, 8, stride=24), :], 127, 1)
            last = pltpu.roll(state_ref[pl.ds(at + 15, 8, stride=24), :], 1, 1)
            state_ref[pl.ds(at + 16, 8, stride=24), :] = jnp.where(band < 7, first, 0.0)
            state_ref[pl.ds(at + 7, 8, stride=24), :] = jnp.where(band > 0, last, 0.0)

    for j in range(2):
        for f in range(FIELDS):
            for at in range(LONS):
                one, two = one_ref[j, f, at], two_ref[j, f, at]
                put(j, f, at, jnp.where(odd, one, two))
                put(j, f, LONS + at, own_ref[j, f, at])
                put(j, f, 2 * LONS + at, jnp.where(odd, two, one))
            edges(j, f, 0, width)

    keep = 1.0 / diffusion - 4.0
    wave = 0.5 * wave_coef / diffusion
    wave_new = 0.5 * wave_coef
    turn = coriolis / diffusion
    unit = diffusion**STEPS
    result = {}
    for step in range(STEPS):
        low, high = 2 * step + 1, width - 2 * step - 1
        for j in range(2):
            p = {col: here(j, 0, col) for col in (low - 1, low)}
            q = {col: here(j, 1, col) for col in (low - 1, low)}
            for col in range(low, high):
                p[col + 1], q[col + 1] = here(j, 0, col + 1), here(j, 1, col + 1)
                p_next, p_last = rows(j, 0, col)
                r_next, r_last = rows(j, 2, col)
                p1 = ((keep * p[col] + (p[col - 1] + p[col + 1])) + (p_next + p_last)) + wave * (
                    (q[col + 1] - q[col - 1]) + (r_next - r_last)
                )
                put(j, 0, col, p1)
            edges(j, 0, low, high)
        low, high = low + 1, high - 1
        for j in range(2):
            p, q, r = (
                {col: here(j, f, col) for col in (low - 1, low)} for f in range(FIELDS)
            )
            for col in range(low, high):
                p[col + 1], q[col + 1], r[col + 1] = (here(j, f, col + 1) for f in range(FIELDS))
                p_next, p_last = rows(j, 0, col)
                q_next, q_last = rows(j, 1, col)
                r_next, r_last = rows(j, 2, col)
                q1 = (
                    (keep * q[col] + (q[col - 1] + q[col + 1])) + (q_next + q_last)
                ) + (wave_new * (p[col + 1] - p[col - 1]) + turn * r[col])
                r1 = (
                    (keep * r[col] + (r[col - 1] + r[col + 1])) + (r_next + r_last)
                ) + (wave_new * (p_next - p_last) - turn * q[col])
                if step < STEPS - 1:
                    put(j, 1, col, q1)
                    put(j, 2, col, r1)
                else:
                    for f, value in enumerate((p[col], q1, r1)):
                        result[j, f, col - LONS] = value
            if step < STEPS - 1:
                edges(j, 1, low, high)
                edges(j, 2, low, high)

    def terms(f, col):
        return [unit * result[j, f, col] - decay_ref[f, col] * own_ref[j, f, col] for j in range(2)]

    chain_first(terms, decay_ref, pairs_ref, carry_ref, weigh_ref)


def emphases(core):
    first = (2 * (iota(1) // 8 + 16 * core)).astype(jnp.float32)
    return [1.0 + 2.0 * (first + j) / 63.0 for j in range(2)]


def so_far_kernel(core_ref, *refs):
    zeros, aboves = refs[0:ITERS], refs[ITERS : 2 * ITERS]
    misfit_ref, out_ref = refs[2 * ITERS :]
    emphasis = emphases(core_ref[0])
    sums = [jnp.zeros((8, 128), jnp.float32) for _ in range(2 * ITERS - 2)]
    for f in range(FIELDS):
        for col in range(LONS):
            for j in range(2):
                parts = [
                    zeros[n][f, col] if j == 0 else aboves[n][0, f, col] for n in range(ITERS)
                ]
                total = parts[0]
                for n in range(1, ITERS):
                    total = total + parts[n]
                    changed, size = emphasis[j] * (parts[n] * parts[n]), emphasis[j] * (total * total)
                    sums[n - 1] = sums[n - 1] + changed
                    sums[ITERS + n - 2] = sums[ITERS + n - 2] + size
                out_ref[(j * FIELDS + f) * LONS + col] = total
    for at, value in enumerate(sums + [misfit_ref[...]]):
        out_ref[CELLS + at] = value


def finish_kernel(
    core_ref,
    pairs_ref,
    other_pairs_ref,
    total_ref,
    other_total_ref,
    decay_ref,
    out_ref,
    weigh_ref,
    carry_ref,
    turn_ref,
    back_ref,
):
    low = core_ref[0] == 0
    pair = iota(1) // 8
    pairs = (pairs_ref, other_pairs_ref)
    totals = (total_ref, other_total_ref)

    def of_half(half, refs, *at):
        mine, other = refs[0][at], refs[1][at]
        return jnp.where(low, mine, other) if half == 0 else jnp.where(low, other, mine)

    chain_first(
        lambda f, col: None,
        decay_ref,
        None,
        carry_ref,
        weigh_ref,
        both_of=lambda f, col: of_half(1, pairs, 0, f, col),
    )
    change = size = jnp.zeros((8, 128), jnp.float32)
    result = {}
    for half in range(2):
        emphasis = emphases(half)
        for f in range(FIELDS):
            for col in range(LONS):
                decay = decay_ref[f, col]
                both, c1 = (of_half(half, pairs, i, f, col) for i in range(2))
                if half == 0:
                    enters = jnp.where(pair == 15, decay * carry_ref[f, col], 0.0)
                    both, c1 = both + decay * enters, c1 + enters
                for j, value in enumerate(chain_local(both, c1, decay, pair)):
                    total = of_half(half, totals, (j * FIELDS + f) * LONS + col) + value
                    change = change + emphasis[j] * (value * value)
                    size = size + emphasis[j] * (total * total)
                    result[half, j, f, col] = total
    row = iota(0)
    sums = [total_ref[CELLS + at] + other_total_ref[CELLS + at] for at in range(2 * ITERS - 1)]
    counted = sums[0 : ITERS - 1] + [change, sums[-1]] + sums[ITERS - 1 : 2 * ITERS - 2] + [size]
    parts = jnp.zeros((8, 128), jnp.float32)
    for at, part in enumerate(counted):
        parts = jnp.where(row == at, jnp.sum(part, axis=0, keepdims=True), parts)
    ones = jnp.ones((128, 128), jnp.float32)
    turn_ref[48:56, :] = jnp.dot(parts, ones, precision=lax.Precision.HIGHEST)
    for half in range(2):
        for s in range(4):
            for side in range(2):
                for j in range(2):
                    for f in range(FIELDS):
                        to = 64 * side + 24 * j + 8 * f
                        turn_ref[to : to + 8, :] = result[half, j, f, s + 4 * side]
            back_ref[...] = turn_ref[...].T
            evens = back_ref[pl.ds(0, 64, stride=2), :]
            odds = back_ref[pl.ds(1, 64, stride=2), :]
            out_ref[pl.ds(256 * half + s, 64, stride=4), :] = jnp.where(low, evens, odds)


def unpack_kernel(in_ref, out_ref, misfit_ref, changes_ref, rows_ref):
    sums = [in_ref[8 * v : 8 * v + 8, :] for v in range(64)]
    while len(sums) > 1:
        sums = [a + b for a, b in zip(sums[::2], sums[1::2])]
    total = pltpu.roll(sums[0] + pltpu.roll(sums[0], 4, 0), 80, 1)
    misfit_ref[...] = total[0:1, 3:4]
    changes_ref[...] = (total / (pltpu.roll(total, 124, 1) + epsilon))[0:1, 0:ITERS]
    second = (lax.broadcasted_iota(jnp.int32, (128, 128), 0) & 7) >= 4
    for b in range(8):
        for i in range(16):
            at = 4 * chip_of(16 * b + i)
            piece = in_ref[at : at + 4, :]
            rows_ref[8 * i : 8 * i + 4, :] = piece
            rows_ref[8 * i + 4 : 8 * i + 8, :] = piece
        block = rows_ref[...]
        turned = jnp.where(second, pltpu.roll(block, 64, 1), block).T
        for j in range(2):
            for f in range(FIELDS):
                at = 24 * j + 8 * f
                out_ref[j, f, :, 128 * b : 128 * b + 128] = turned[at : at + 8, :]


def per_device(departure, obs_weight, obs_block, coarse_decay):
    z, y, x, core = (lax.axis_index(name) for name in ("z", "y", "x", "c"))
    core_arg = core.astype(jnp.int32).reshape(1)
    tile_odd = ((x + y + z + core) % 2).astype(jnp.int32).reshape(1)
    place = (z * NY + y).astype(jnp.int32).reshape(1)

    position = ((z * NY + y) * 2 + jnp.arange(2)).astype(jnp.float32)
    strength = (1.0 + 2.0 * position / 63.0)[:, None] * obs_weight
    misfit_part = 0.5 * jnp.sum(
        strength[:, :, None, None] * departure * departure, axis=(0, 1, 2)
    ).reshape(8, 128)

    sent = call(
        pack_kernel,
        shape(512, 128),
        (place,),
        far=(departure.transpose(0, 2, 1, 3), obs_weight, obs_block, coarse_decay),
        scratch=[
            pltpu.VMEM((2, FIELDS, 16, 1024), jnp.float32),
            pltpu.VMEM((2, 16), jnp.float32),
            pltpu.VMEM((2, 16), jnp.int32),
            pltpu.VMEM((FIELDS, 8, 1024), jnp.float32),
            pltpu.VMEM((512, 128), jnp.float32),
            pltpu.SemaphoreType.DMA((4,)),
        ],
    )
    got = lax.all_to_all(sent.reshape(CHIPS, 4, 128), ZYX, 0, 0).reshape(512, 128)
    other = lax.ppermute(got, "c", SIBLING)

    field = shape(FIELDS, LONS, 8, 128)
    both = shape(2, FIELDS, LONS, 8, 128)
    square = pltpu.VMEM((128, 128), jnp.float32)
    weigh = pltpu.VMEM((FIELDS * LONS * 8, 128), jnp.float32)
    zero, above, decay, power = call(
        open_kernel,
        (field, both, field, both),
        (core_arg,),
        got,
        other,
        scratch=[
            square,
            pltpu.VMEM((2, 2, FIELDS, LONS, 8, 128), jnp.float32),
            weigh,
            pltpu.VMEM((FIELDS, LONS, 8, 128), jnp.float32),
        ],
    )
    zeros, aboves = [], []
    for iteration in range(ITERS):
        if iteration > 0:
            zero, above = call(
                close_kernel, (field, both), (core_arg,), first, second, carry, power
            )
        zeros.append(zero)
        aboves.append(above)
        side_one = lax.ppermute(above, ALL, swap_pairs(0))
        side_two = lax.ppermute(above, ALL, swap_pairs(1))
        last = iteration == ITERS - 1
        found = call(
            fine_kernel,
            both if last else (both, field),
            (tile_odd,),
            above,
            side_one,
            side_two,
            decay,
            scratch=[pltpu.VMEM((2 * FIELDS * 3 * LONS * 24, 128), jnp.float32)]
            + ([] if last else [weigh]),
        )
        pairs, carry = (found, None) if last else found
        if not last:
            carry = lax.ppermute(carry, "c", SIBLING)
            first, second = call(scan_kernel, (field, field), (), pairs, decay)
    total = call(
        so_far_kernel,
        shape(CELLS + 2 * ITERS - 1, 8, 128),
        (core_arg,),
        *zeros,
        *aboves,
        misfit_part,
    )
    other_total, other_pairs = (lax.ppermute(value, "c", SIBLING) for value in (total, pairs))
    back = call(
        finish_kernel,
        shape(512, 128),
        (core_arg,),
        pairs,
        other_pairs,
        total,
        other_total,
        decay,
        scratch=[weigh, pltpu.VMEM((FIELDS, LONS, 8, 128), jnp.float32), square, square],
    )
    home = lax.all_to_all(back.reshape(CHIPS, 4, 128), ZYX, 0, 0).reshape(512, 128)
    adjoint, misfit, changes = call(
        unpack_kernel,
        (
            jax.ShapeDtypeStruct((2, FIELDS, 8, 1024), jnp.float32),
            jax.ShapeDtypeStruct((1, 1), jnp.float32),
            jax.ShapeDtypeStruct((1, ITERS), jnp.float32),
        ),
        (),
        home,
        scratch=[square],
    )
    return adjoint, misfit.reshape(()), changes.reshape(ITERS)


def solution(mesh):
    split = Mesh(mesh.devices.reshape(NZ, NY, NX, 2), ("z", "y", "x", "c"))
    return jax.shard_map(
        per_device,
        mesh=split,
        in_specs=(P(TM, GRID, None, None), P(TM, GRID), P(TM, GRID), P(None, GRID, None)),
        out_specs=(P(TM, None, GRID, None), P(), P()),
        check_vma=False,
    )
```

```python
import functools

import jax
import jax.numpy as jnp
from jax import lax
from jax.experimental import pallas as pl
from jax.experimental.pallas import tpu as pltpu
from jax.sharding import Mesh
from jax.sharding import PartitionSpec as P

STEPS = 4
ITERS = 3
NZ, NY, NX = 8, 4, 4
CHIPS = NZ * NY * NX
LONS = 8
FIELDS = 3
CELLS = 2 * FIELDS * LONS
TM = ("z", "y")
GRID = ("x", "c")
ZYX = ("z", "y", "x")
ALL = ("z", "y", "x", "c")

wave_coef = 0.6
diffusion = 0.05
coriolis = 0.1
epsilon = 1e-06


def chip_of(tile):
    z, place = divmod(tile, NY * NX)
    if z % 2:
        place = NY * NX - 1 - place
    y, x = divmod(place, NX)
    if y % 2:
        x = NX - 1 - x
    return (z * NY + y) * NX + x


def swap_pairs(first):
    pairs = []
    for tile in range(CHIPS):
        core = (tile + first) % 2
        a, b = 2 * chip_of(tile) + core, 2 * chip_of((tile + 1) % CHIPS) + core
        pairs += [(a, b), (b, a)]
    return pairs


SIBLING = [(0, 1), (1, 0)]


def shape(*dims):
    return pltpu.VMEM(dims, jnp.float32)


def near(value):
    return pltpu.with_memory_space_constraint(value, pltpu.VMEM)


def call(kernel, outs, scalars, *operands, far=(), scratch=()):
    vmem = pl.BlockSpec(memory_space=pltpu.VMEM)
    hbm = pl.BlockSpec(memory_space=pl.ANY)
    smem = pl.BlockSpec(memory_space=pltpu.SMEM)
    outs = outs if isinstance(outs, tuple) else (outs,)
    results = pl.pallas_call(
        kernel,
        out_shape=outs,
        in_specs=[smem] * len(scalars) + [hbm] * len(far) + [vmem] * len(operands),
        out_specs=[vmem] * len(outs),
        scratch_shapes=list(scratch),
    )(*scalars, *far, *map(near, operands))
    return results if len(outs) > 1 else results[0]


def iota(dim):
    return lax.broadcasted_iota(jnp.int32, (8, 128), dim)


def split(values):
    high = values.astype(jnp.bfloat16)
    return high, (values - high.astype(jnp.float32)).astype(jnp.bfloat16)


def pack_kernel(
    place_ref,
    departure_ref,
    weight_ref,
    block_ref,
    decay_ref,
    out_ref,
    values_ref,
    weights_ref,
    blocks_ref,
    decays_ref,
    rows_ref,
    sems,
):
    copies = [
        pltpu.make_async_copy(weight_ref, weights_ref, sems.at[0]),
        pltpu.make_async_copy(block_ref, blocks_ref, sems.at[1]),
        pltpu.make_async_copy(departure_ref.at[0], values_ref.at[0], sems.at[2]),
        pltpu.make_async_copy(departure_ref.at[1], values_ref.at[1], sems.at[3]),
        pltpu.make_async_copy(decay_ref, decays_ref, sems.at[4]),
    ]
    for copy in copies:
        copy.start()
    for copy in copies[:3]:
        copy.wait()
    block = lax.broadcasted_iota(jnp.int32, (8, 16), 0)
    for j in range(2):
        if j == 1:
            for copy in copies[3:]:
                copy.wait()
        emphasis = 1.0 + 2.0 * (place_ref[0] * 2 + j).astype(jnp.float32) / 63.0
        choose = jnp.where(
            blocks_ref[j : j + 1, :] == block, emphasis * weights_ref[j : j + 1, :], 0.0
        )
        choose_high, choose_low = split(choose)
        choose_both = jnp.concatenate([choose_high, choose_low], axis=0)
        for f in range(FIELDS):
            values_high, values_low = split(values_ref[j, f])
            main = jnp.dot(choose_both, values_high, preferred_element_type=jnp.float32)
            rest = jnp.dot(choose_high, values_low, preferred_element_type=jnp.float32)
            tiles = main[0:8] + (main[8:16] + rest)
            for r in range(8):
                rows_ref[pl.ds(24 * j + 8 * f + r, 8, stride=64), :] = tiles[
                    :, 128 * r : 128 * r + 128
                ]
    odd = (place_ref[0] & 1) == 1
    for b in range(8):
        span = slice(128 * b, 128 * b + 128)
        rows_ref[64 * b + 48 : 64 * b + 56, :] = jnp.where(
            odd, decays_ref[2, :, span], decays_ref[0, :, span]
        )
        rows_ref[64 * b + 56 : 64 * b + 64, :] = decays_ref[1, :, span]
    for b in range(8):
        block = rows_ref[64 * b : 64 * b + 64, :]
        both = jnp.concatenate([block, pltpu.roll(block, 124, 1)], axis=0)
        turned = both.T
        for i in range(16):
            to = 4 * chip_of(16 * b + i)
            out_ref[to : to + 4, :] = turned[8 * i : 8 * i + 4, :]


def later(value, groups):
    return pltpu.roll(value, 128 - 8 * groups, value.ndim - 1)


def scan_pairs(u, square, pair):
    for groups in (1, 4):
        factor = square
        total = u
        for times in (1, 2, 3):
            back = times * groups
            total = total + jnp.where(pair < 16 - back, factor, 0.0) * later(u, back)
            factor = factor * square
        u, square = total, factor
    return u


def bands_summed(values):
    source = lax.broadcasted_iota(jnp.int32, (128, 128), 0)
    target = lax.broadcasted_iota(jnp.int32, (128, 128), 1)
    same = (source % 8 == target % 8).astype(jnp.float32)
    return jnp.dot(
        values, same, precision=lax.Precision.HIGHEST, preferred_element_type=jnp.float32
    )


def chain_first(terms_of, decay_ref, pairs_ref, carry_ref, weigh_ref, both_of=None):
    pair = iota(1) // 8
    for f in range(FIELDS):
        for col in range(LONS):
            decay = decay_ref[f, col]
            if both_of is None:
                c0, c1 = terms_of(f, col)
                both = c0 + decay * c1
            else:
                both = both_of(f, col)
            if pairs_ref is not None:
                pairs_ref[0, f, col] = both
                pairs_ref[1, f, col] = c1
            if carry_ref is not None:
                at = 8 * (LONS * f + col)
                weigh_ref[at : at + 8, :] = powers(decay * decay, pair, (1, 2, 4, 8)) * both
    if carry_ref is not None:
        carry_ref[...] = bands_summed(weigh_ref[...]).reshape(FIELDS, LONS, 8, 128)


def chain_local(both, c1, decay, pair):
    value = scan_pairs(both, decay * decay, pair)
    return value, c1 + decay * jnp.where(pair < 15, later(value, 1), 0.0)


def scan_kernel(pairs_ref, decay_ref, first_ref, second_ref):
    pair = iota(1) // 8
    for f in range(FIELDS):
        for col in range(LONS):
            first_ref[f, col], second_ref[f, col] = chain_local(
                pairs_ref[0, f, col], pairs_ref[1, f, col], decay_ref[f, col], pair
            )


def powers(square, exponent, bits=(1, 2, 4, 8, 16)):
    power = jnp.where((exponent & 1) != 0, square, 1.0)
    for bit in bits[1:]:
        square = square * square
        power = power * jnp.where((exponent & bit) != 0, square, 1.0)
    return power


def send_halo(odd_ref, above_ref, one_ref, two_ref):
    odd = odd_ref[0] == 1
    for j in range(2):
        for f in range(FIELDS - 1):
            for col in range(LONS):
                one_ref[j, LONS * f + col] = two_ref[j, LONS * f + col] = above_ref[j, f, col]
        for col in range(LONS - 1):
            near_west, near_east = above_ref[j, 2, col], above_ref[j, 2, col + 1]
            at = LONS * (FIELDS - 1) + col
            one_ref[j, at] = jnp.where(odd, near_west, near_east)
            two_ref[j, at] = jnp.where(odd, near_east, near_west)


def open_kernel(
    core_ref,
    odd_ref,
    mine_ref,
    other_ref,
    zero_ref,
    above_ref,
    one_ref,
    two_ref,
    decay_ref,
    power_ref,
    turn_ref,
    terms_ref,
    weigh_ref,
    carry_ref,
):
    low = core_ref[0] == 0
    lane = iota(1)
    pair = lane // 8
    even = (pair & 1) == 0

    def turned(half_ref, s):
        turn_ref[pl.ds(0, 64, stride=2), :] = jnp.where(low, half_ref[0], half_ref[1])
        turn_ref[pl.ds(1, 64, stride=2), :] = jnp.where(low, half_ref[1], half_ref[0])
        return turn_ref[...].T

    for s in range(4):
        early, late = (
            [ref[pl.ds(at + s, 64, stride=4), :] for ref in (mine_ref, other_ref)]
            for at in (0, 256)
        )
        here = turned([jnp.where(low, a, b) for a, b in zip(early, late)], s)
        behind = turned(late, s)
        for half in range(2):
            at = 64 * half
            col = s + 4 * half
            mixed = here[at + 48 : at + 56, :]
            decays = (
                jnp.where(even, mixed, pltpu.roll(mixed, 8, 1)),
                here[at + 56 : at + 64, :],
                jnp.where(even, pltpu.roll(mixed, 120, 1), mixed),
            )
            for f in range(FIELDS):
                decay = decays[f]
                decay_ref[f, col] = decay
                for j in range(2):
                    to = at + 24 * j + 8 * f
                    terms_ref[0, j, f, col] = here[to : to + 8, :]
                    terms_ref[1, j, f, col] = behind[to : to + 8, :]
                square = decay * decay
                power_ref[0, f, col] = powers(square, 16 - pair)
                power_ref[1, f, col] = decay * powers(square, 15 - pair, (1, 2, 4, 8))
    chain_first(
        lambda f, col: (terms_ref[1, 0, f, col], terms_ref[1, 1, f, col]),
        decay_ref,
        None,
        carry_ref,
        weigh_ref,
    )
    for f in range(FIELDS):
        for col in range(LONS):
            decay = decay_ref[f, col]
            c0, c1 = terms_ref[0, 0, f, col], terms_ref[0, 1, f, col]
            carry = jnp.where(low, carry_ref[f, col], 0.0)
            c1 = c1 + jnp.where(pair == 15, decay * carry, 0.0)
            value, second = chain_local(c0 + decay * c1, c1, decay, pair)
            zero_ref[f, col] = value
            above_ref[0, f, col] = second
            above_ref[1, f, col] = jnp.where(pair < 15, later(value, 1), carry)
    send_halo(odd_ref, above_ref, one_ref, two_ref)


def close_kernel(
    core_ref,
    odd_ref,
    first_ref,
    second_ref,
    carry_ref,
    power_ref,
    zero_ref,
    above_ref,
    one_ref,
    two_ref,
):
    low = core_ref[0] == 0
    pair = iota(1) // 8
    for f in range(FIELDS):
        for col in range(LONS):
            carry = jnp.where(low, carry_ref[f, col], 0.0)
            value = first_ref[f, col] + power_ref[0, f, col] * carry
            zero_ref[f, col] = value
            above_ref[0, f, col] = second_ref[f, col] + power_ref[1, f, col] * carry
            above_ref[1, f, col] = jnp.where(pair < 15, later(value, 1), carry)
    send_halo(odd_ref, above_ref, one_ref, two_ref)


def fine_kernel(
    odd_ref, own_ref, one_ref, two_ref, decay_ref, pairs_ref, *rest
):
    carry_ref, state_ref, weigh_ref = rest if len(rest) == 3 else (None, *rest, None)
    odd = odd_ref[0] == 1
    lane = iota(1)
    band = lane % 8
    width = 3 * LONS

    def slot(j, f, col):
        return 24 * ((j * FIELDS + f) * width + col)

    def put(j, f, col, value):
        at = slot(j, f, col) + 8
        state_ref[at : at + 8, :] = value

    def here(j, f, col):
        at = slot(j, f, col) + 8
        return state_ref[at : at + 8, :]

    def rows(j, f, col):
        at = slot(j, f, col) + 8
        return state_ref[at + 1 : at + 9, :], state_ref[at - 1 : at + 7, :]

    def edges(j, f, low, high):
        for col in range(low, high, 8):
            at = slot(j, f, min(col, width - 8))
            first = pltpu.roll(state_ref[pl.ds(at + 8, 8, stride=24), :], 127, 1)
            last = pltpu.roll(state_ref[pl.ds(at + 15, 8, stride=24), :], 1, 1)
            state_ref[pl.ds(at + 16, 8, stride=24), :] = jnp.where(band < 7, first, 0.0)
            state_ref[pl.ds(at + 7, 8, stride=24), :] = jnp.where(band > 0, last, 0.0)

    for j in range(2):
        for f in range(FIELDS):
            skipped = 1 if f == 2 else 0
            for at in range(LONS - skipped):
                one, two = one_ref[j, LONS * f + at], two_ref[j, LONS * f + at]
                put(j, f, at + skipped, jnp.where(odd, one, two))
                put(j, f, 2 * LONS + at, jnp.where(odd, two, one))
            for at in range(LONS):
                put(j, f, LONS + at, own_ref[j, f, at])
            if skipped:
                put(j, f, 0, jnp.zeros((8, 128), jnp.float32))
                put(j, f, width - 1, jnp.zeros((8, 128), jnp.float32))
            edges(j, f, 0, width)

    keep = 1.0 / diffusion - 4.0
    wave = 0.5 * wave_coef / diffusion
    wave_new = 0.5 * wave_coef
    turn = coriolis / diffusion
    unit = diffusion**STEPS
    result = {}
    for step in range(STEPS):
        low, high = 2 * step + 1, width - 2 * step - 1
        for j in range(2):
            p = {col: here(j, 0, col) for col in (low - 1, low)}
            q = {col: here(j, 1, col) for col in (low - 1, low)}
            for col in range(low, high):
                p[col + 1], q[col + 1] = here(j, 0, col + 1), here(j, 1, col + 1)
                p_next, p_last = rows(j, 0, col)
                r_next, r_last = rows(j, 2, col)
                p1 = ((keep * p[col] + (p[col - 1] + p[col + 1])) + (p_next + p_last)) + wave * (
                    (q[col + 1] - q[col - 1]) + (r_next - r_last)
                )
                put(j, 0, col, p1)
            edges(j, 0, low, high)
        low, high = low + 1, high - 1
        for j in range(2):
            p, q, r = (
                {col: here(j, f, col) for col in (low - 1, low)} for f in range(FIELDS)
            )
            for col in range(low, high):
                p[col + 1], q[col + 1], r[col + 1] = (here(j, f, col + 1) for f in range(FIELDS))
                p_next, p_last = rows(j, 0, col)
                q_next, q_last = rows(j, 1, col)
                r_next, r_last = rows(j, 2, col)
                q1 = (
                    (keep * q[col] + (q[col - 1] + q[col + 1])) + (q_next + q_last)
                ) + (wave_new * (p[col + 1] - p[col - 1]) + turn * r[col])
                r1 = (
                    (keep * r[col] + (r[col - 1] + r[col + 1])) + (r_next + r_last)
                ) + (wave_new * (p_next - p_last) - turn * q[col])
                if step < STEPS - 1:
                    put(j, 1, col, q1)
                    if low < col < high - 1:
                        put(j, 2, col, r1)
                else:
                    for f, value in enumerate((p[col], q1, r1)):
                        result[j, f, col - LONS] = value
            if step < STEPS - 1:
                edges(j, 1, low, high)
                edges(j, 2, low, high)

    def terms(f, col):
        return [unit * result[j, f, col] - decay_ref[f, col] * own_ref[j, f, col] for j in range(2)]

    chain_first(terms, decay_ref, pairs_ref, carry_ref, weigh_ref)


def emphases(core):
    first = (2 * (iota(1) // 8 + 16 * core)).astype(jnp.float32)
    return [1.0 + 2.0 * (first + j) / 63.0 for j in range(2)]


def so_far_kernel(core_ref, *refs):
    zeros, aboves = refs[0:ITERS], refs[ITERS : 2 * ITERS]
    misfit_ref, out_ref = refs[2 * ITERS :]
    emphasis = emphases(core_ref[0])
    sums = [jnp.zeros((8, 128), jnp.float32) for _ in range(2 * ITERS - 2)]
    for f in range(FIELDS):
        for col in range(LONS):
            for j in range(2):
                parts = [
                    zeros[n][f, col] if j == 0 else aboves[n][0, f, col] for n in range(ITERS)
                ]
                total = parts[0]
                for n in range(1, ITERS):
                    total = total + parts[n]
                    changed, size = emphasis[j] * (parts[n] * parts[n]), emphasis[j] * (total * total)
                    sums[n - 1] = sums[n - 1] + changed
                    sums[ITERS + n - 2] = sums[ITERS + n - 2] + size
                out_ref[(j * FIELDS + f) * LONS + col] = total
    for at, value in enumerate(sums + [misfit_ref[...]]):
        out_ref[CELLS + at] = value


def finish_kernel(
    core_ref,
    first_ref,
    second_ref,
    pairs_ref,
    other_pairs_ref,
    total_ref,
    other_total_ref,
    decay_ref,
    power_ref,
    out_ref,
    weigh_ref,
    carry_ref,
    turn_ref,
    back_ref,
):
    low = core_ref[0] == 0
    pair = iota(1) // 8
    chain_first(
        lambda f, col: None,
        decay_ref,
        None,
        carry_ref,
        weigh_ref,
        both_of=lambda f, col: jnp.where(low, other_pairs_ref[0, f, col], pairs_ref[0, f, col]),
    )
    change = size = jnp.zeros((8, 128), jnp.float32)
    result = {}
    emphasis = emphases(core_ref[0]), emphases(1 - core_ref[0])
    for f in range(FIELDS):
        for col in range(LONS):
            decay, carry = decay_ref[f, col], carry_ref[f, col]
            mine, others = jnp.where(low, carry, 0.0), jnp.where(low, 0.0, carry)
            enters = jnp.where(pair == 15, decay * others, 0.0)
            values = (
                (
                    first_ref[f, col] + power_ref[0, f, col] * mine,
                    second_ref[f, col] + power_ref[1, f, col] * mine,
                ),
                chain_local(
                    other_pairs_ref[0, f, col] + decay * enters,
                    other_pairs_ref[1, f, col] + enters,
                    decay,
                    pair,
                ),
            )
            for side, ref in enumerate((total_ref, other_total_ref)):
                for j in range(2):
                    value = values[side][j]
                    total = ref[(j * FIELDS + f) * LONS + col] + value
                    change = change + emphasis[side][j] * (value * value)
                    size = size + emphasis[side][j] * (total * total)
                    result[side, j, f, col] = total
    row = iota(0)
    sums = [total_ref[CELLS + at] + other_total_ref[CELLS + at] for at in range(2 * ITERS - 1)]
    counted = sums[0 : ITERS - 1] + [change, sums[-1]] + sums[ITERS - 1 : 2 * ITERS - 2] + [size]
    parts = jnp.zeros((8, 128), jnp.float32)
    for at, part in enumerate(counted):
        parts = jnp.where(row == at, jnp.sum(part, axis=0, keepdims=True), parts)
    ones = jnp.ones((128, 128), jnp.float32)
    turn_ref[48:56, :] = jnp.dot(parts, ones, precision=lax.Precision.HIGHEST)
    for s in range(4):
        kept = []
        for which in range(2):
            for side in range(2):
                for j in range(2):
                    for f in range(FIELDS):
                        to = 64 * side + 24 * j + 8 * f
                        turn_ref[to : to + 8, :] = result[which, j, f, s + 4 * side]
            back_ref[...] = turn_ref[...].T
            evens = back_ref[pl.ds(0, 64, stride=2), :]
            odds = back_ref[pl.ds(1, 64, stride=2), :]
            kept.append(jnp.where(low, evens, odds))
        out_ref[pl.ds(s, 64, stride=4), :] = jnp.where(low, kept[0], kept[1])
        out_ref[pl.ds(256 + s, 64, stride=4), :] = jnp.where(low, kept[1], kept[0])


def unpack_kernel(in_ref, out_ref, misfit_ref, changes_ref, rows_ref):
    sums = [in_ref[8 * v : 8 * v + 8, :] for v in range(64)]
    while len(sums) > 1:
        sums = [a + b for a, b in zip(sums[::2], sums[1::2])]
    total = pltpu.roll(sums[0] + pltpu.roll(sums[0], 4, 0), 80, 1)
    misfit_ref[...] = total[0:1, 3:4]
    changes_ref[...] = (total / (pltpu.roll(total, 124, 1) + epsilon))[0:1, 0:ITERS]
    second = (lax.broadcasted_iota(jnp.int32, (128, 128), 0) & 7) >= 4
    for b in range(8):
        for i in range(16):
            at = 4 * chip_of(16 * b + i)
            piece = in_ref[at : at + 4, :]
            rows_ref[8 * i : 8 * i + 4, :] = piece
            rows_ref[8 * i + 4 : 8 * i + 8, :] = piece
        block = rows_ref[...]
        turned = jnp.where(second, pltpu.roll(block, 64, 1), block).T
        for j in range(2):
            for f in range(FIELDS):
                at = 24 * j + 8 * f
                out_ref[j, f, :, 128 * b : 128 * b + 128] = turned[at : at + 8, :]


def per_device(departure, obs_weight, obs_block, coarse_decay):
    z, y, x, core = (lax.axis_index(name) for name in ("z", "y", "x", "c"))
    core_arg = core.astype(jnp.int32).reshape(1)
    tile_odd = ((x + y + z + core) % 2).astype(jnp.int32).reshape(1)
    place = (z * NY + y).astype(jnp.int32).reshape(1)

    position = ((z * NY + y) * 2 + jnp.arange(2)).astype(jnp.float32)
    strength = (1.0 + 2.0 * position / 63.0)[:, None] * obs_weight
    misfit_part = 0.5 * jnp.sum(
        strength[:, :, None, None] * departure * departure, axis=(0, 1, 2)
    ).reshape(8, 128)

    sent = call(
        pack_kernel,
        shape(512, 128),
        (place,),
        far=(departure.transpose(0, 2, 1, 3), obs_weight, obs_block, coarse_decay),
        scratch=[
            pltpu.VMEM((2, FIELDS, 16, 1024), jnp.float32),
            pltpu.VMEM((2, 16), jnp.float32),
            pltpu.VMEM((2, 16), jnp.int32),
            pltpu.VMEM((FIELDS, 8, 1024), jnp.float32),
            pltpu.VMEM((512, 128), jnp.float32),
            pltpu.SemaphoreType.DMA((5,)),
        ],
    )
    got = lax.all_to_all(sent.reshape(CHIPS, 4, 128), ZYX, 0, 0).reshape(512, 128)
    other = lax.ppermute(got, "c", SIBLING)

    field = shape(FIELDS, LONS, 8, 128)
    both = shape(2, FIELDS, LONS, 8, 128)
    square = pltpu.VMEM((128, 128), jnp.float32)
    weigh = pltpu.VMEM((FIELDS * LONS * 8, 128), jnp.float32)
    halo = shape(2, LONS * FIELDS - 1, 8, 128)
    zero, above, to_one, to_two, decay, power = call(
        open_kernel,
        (field, both, halo, halo, field, both),
        (core_arg, tile_odd),
        got,
        other,
        scratch=[
            square,
            pltpu.VMEM((2, 2, FIELDS, LONS, 8, 128), jnp.float32),
            weigh,
            pltpu.VMEM((FIELDS, LONS, 8, 128), jnp.float32),
        ],
    )
    zeros, aboves = [], []
    for iteration in range(ITERS):
        if iteration > 0:
            zero, above, to_one, to_two = call(
                close_kernel,
                (field, both, halo, halo),
                (core_arg, tile_odd),
                first,
                second,
                carry,
                power,
            )
        zeros.append(zero)
        aboves.append(above)
        side_one = lax.ppermute(to_one, ALL, swap_pairs(0))
        side_two = lax.ppermute(to_two, ALL, swap_pairs(1))
        last = iteration == ITERS - 1
        found = call(
            fine_kernel,
            both if last else (both, field),
            (tile_odd,),
            above,
            side_one,
            side_two,
            decay,
            scratch=[pltpu.VMEM((2 * FIELDS * 3 * LONS * 24, 128), jnp.float32)]
            + ([] if last else [weigh]),
        )
        pairs, carry = (found, None) if last else found
        if not last:
            carry = lax.ppermute(carry, "c", SIBLING)
        first, second = call(scan_kernel, (field, field), (), pairs, decay)
    total = call(
        so_far_kernel,
        shape(CELLS + 2 * ITERS - 1, 8, 128),
        (core_arg,),
        *zeros,
        *aboves,
        misfit_part,
    )
    other_total, other_pairs = (lax.ppermute(value, "c", SIBLING) for value in (total, pairs))
    back = call(
        finish_kernel,
        shape(512, 128),
        (core_arg,),
        first,
        second,
        pairs,
        other_pairs,
        total,
        other_total,
        decay,
        power,
        scratch=[weigh, pltpu.VMEM((FIELDS, LONS, 8, 128), jnp.float32), square, square],
    )
    home = lax.all_to_all(back.reshape(CHIPS, 4, 128), ZYX, 0, 0).reshape(512, 128)
    adjoint, misfit, changes = call(
        unpack_kernel,
        (
            jax.ShapeDtypeStruct((2, FIELDS, 8, 1024), jnp.float32),
            jax.ShapeDtypeStruct((1, 1), jnp.float32),
            jax.ShapeDtypeStruct((1, ITERS), jnp.float32),
        ),
        (),
        home,
        scratch=[square],
    )
    return adjoint, misfit.reshape(()), changes.reshape(ITERS)


def solution(mesh):
    split = Mesh(mesh.devices.reshape(NZ, NY, NX, 2), ("z", "y", "x", "c"))
    return jax.shard_map(
        per_device,
        mesh=split,
        in_specs=(P(TM, GRID, None, None), P(TM, GRID), P(TM, GRID), P(None, GRID, None)),
        out_specs=(P(TM, None, GRID, None), P(), P()),
        check_vma=False,
    )
```

```python
import functools

import jax
import jax.numpy as jnp
from jax import lax
from jax.experimental import pallas as pl
from jax.experimental.pallas import tpu as pltpu
from jax.sharding import Mesh
from jax.sharding import PartitionSpec as P

STEPS = 4
ITERS = 3
NZ, NY, NX = 8, 4, 4
CHIPS = NZ * NY * NX
LONS = 8
FIELDS = 3
CELLS = 2 * FIELDS * LONS
TM = ("z", "y")
GRID = ("x", "c")
ZYX = ("z", "y", "x")
ALL = ("z", "y", "x", "c")

wave_coef = 0.6
diffusion = 0.05
coriolis = 0.1
epsilon = 1e-06


def chip_of(tile):
    z, place = divmod(tile, NY * NX)
    if z % 2:
        place = NY * NX - 1 - place
    y, x = divmod(place, NX)
    if y % 2:
        x = NX - 1 - x
    return (z * NY + y) * NX + x


def swap_pairs(first):
    pairs = []
    for tile in range(CHIPS):
        core = (tile + first) % 2
        a, b = 2 * chip_of(tile) + core, 2 * chip_of((tile + 1) % CHIPS) + core
        pairs += [(a, b), (b, a)]
    return pairs


SIBLING = [(0, 1), (1, 0)]


def shape(*dims):
    return pltpu.VMEM(dims, jnp.float32)


def near(value):
    return pltpu.with_memory_space_constraint(value, pltpu.VMEM)


def call(kernel, outs, scalars, *operands, far=(), scratch=()):
    vmem = pl.BlockSpec(memory_space=pltpu.VMEM)
    hbm = pl.BlockSpec(memory_space=pl.ANY)
    smem = pl.BlockSpec(memory_space=pltpu.SMEM)
    outs = outs if isinstance(outs, tuple) else (outs,)
    results = pl.pallas_call(
        kernel,
        out_shape=outs,
        in_specs=[smem] * len(scalars) + [hbm] * len(far) + [vmem] * len(operands),
        out_specs=[vmem] * len(outs),
        scratch_shapes=list(scratch),
    )(*scalars, *far, *map(near, operands))
    return results if len(outs) > 1 else results[0]


def iota(dim):
    return lax.broadcasted_iota(jnp.int32, (8, 128), dim)


def split(values):
    high = values.astype(jnp.bfloat16)
    return high, (values - high.astype(jnp.float32)).astype(jnp.bfloat16)


def pack_kernel(
    place_ref,
    departure_ref,
    weight_ref,
    block_ref,
    decay_ref,
    out_ref,
    values_ref,
    weights_ref,
    blocks_ref,
    decays_ref,
    rows_ref,
    sems,
):
    copies = [
        pltpu.make_async_copy(weight_ref, weights_ref, sems.at[0]),
        pltpu.make_async_copy(block_ref, blocks_ref, sems.at[1]),
        pltpu.make_async_copy(departure_ref, values_ref, sems.at[2]),
        pltpu.make_async_copy(decay_ref, decays_ref, sems.at[3]),
    ]
    for copy in copies:
        copy.start()
    for copy in copies:
        copy.wait()
    block = lax.broadcasted_iota(jnp.int32, (8, 16), 0)
    for j in range(2):
        emphasis = 1.0 + 2.0 * (place_ref[0] * 2 + j).astype(jnp.float32) / 63.0
        choose = jnp.where(
            blocks_ref[j : j + 1, :] == block, emphasis * weights_ref[j : j + 1, :], 0.0
        )
        choose_high, choose_low = split(choose)
        choose_both = jnp.concatenate([choose_high, choose_low], axis=0)
        for f in range(FIELDS):
            values_high, values_low = split(values_ref[j, f])
            main = jnp.dot(choose_both, values_high, preferred_element_type=jnp.float32)
            rest = jnp.dot(choose_high, values_low, preferred_element_type=jnp.float32)
            tiles = main[0:8] + (main[8:16] + rest)
            for r in range(8):
                rows_ref[pl.ds(24 * j + 8 * f + r, 8, stride=64), :] = tiles[
                    :, 128 * r : 128 * r + 128
                ]
    odd = (place_ref[0] & 1) == 1
    for b in range(8):
        span = slice(128 * b, 128 * b + 128)
        rows_ref[64 * b + 48 : 64 * b + 56, :] = jnp.where(
            odd, decays_ref[2, :, span], decays_ref[0, :, span]
        )
        rows_ref[64 * b + 56 : 64 * b + 64, :] = decays_ref[1, :, span]
    for b in range(8):
        block = rows_ref[64 * b : 64 * b + 64, :]
        both = jnp.concatenate([block, pltpu.roll(block, 124, 1)], axis=0)
        turned = both.T
        for i in range(16):
            to = 4 * chip_of(16 * b + i)
            out_ref[to : to + 4, :] = turned[8 * i : 8 * i + 4, :]


def later(value, groups):
    return pltpu.roll(value, 128 - 8 * groups, value.ndim - 1)


def scan_pairs(u, square, pair):
    for groups in (1, 4):
        factor = square
        total = u
        for times in (1, 2, 3):
            back = times * groups
            total = total + jnp.where(pair < 16 - back, factor, 0.0) * later(u, back)
            factor = factor * square
        u, square = total, factor
    return u


def bands_summed(values):
    source = lax.broadcasted_iota(jnp.int32, (128, 128), 0)
    target = lax.broadcasted_iota(jnp.int32, (128, 128), 1)
    same = (source % 8 == target % 8).astype(jnp.float32)
    return jnp.dot(
        values, same, precision=lax.Precision.HIGHEST, preferred_element_type=jnp.float32
    )


def chain_first(terms_of, decay_ref, pairs_ref, carry_ref, weigh_ref, both_of=None):
    pair = iota(1) // 8
    for f in range(FIELDS):
        for col in range(LONS):
            decay = decay_ref[f, col]
            if both_of is None:
                c0, c1 = terms_of(f, col)
                both = c0 + decay * c1
            else:
                both = both_of(f, col)
            if pairs_ref is not None:
                pairs_ref[0, f, col] = both
                pairs_ref[1, f, col] = c1
            if carry_ref is not None:
                at = 8 * (LONS * f + col)
                weigh_ref[at : at + 8, :] = powers(decay * decay, pair, (1, 2, 4, 8)) * both
    if carry_ref is not None:
        carry_ref[...] = bands_summed(weigh_ref[...]).reshape(FIELDS, LONS, 8, 128)


def chain_local(both, c1, decay, pair):
    value = scan_pairs(both, decay * decay, pair)
    return value, c1 + decay * jnp.where(pair < 15, later(value, 1), 0.0)


def scan_kernel(pairs_ref, decay_ref, first_ref, second_ref):
    pair = iota(1) // 8
    for f in range(FIELDS):
        for col in range(LONS):
            first_ref[f, col], second_ref[f, col] = chain_local(
                pairs_ref[0, f, col], pairs_ref[1, f, col], decay_ref[f, col], pair
            )


def powers(square, exponent, bits=(1, 2, 4, 8, 16)):
    power = jnp.where((exponent & 1) != 0, square, 1.0)
    for bit in bits[1:]:
        square = square * square
        power = power * jnp.where((exponent & bit) != 0, square, 1.0)
    return power


def send_halo(odd_ref, above_ref, one_ref, two_ref):
    odd = odd_ref[0] == 1
    for j in range(2):
        for f in range(FIELDS - 1):
            for col in range(LONS):
                one_ref[j, LONS * f + col] = two_ref[j, LONS * f + col] = above_ref[j, f, col]
        for col in range(LONS - 1):
            near_west, near_east = above_ref[j, 2, col], above_ref[j, 2, col + 1]
            at = LONS * (FIELDS - 1) + col
            one_ref[j, at] = jnp.where(odd, near_west, near_east)
            two_ref[j, at] = jnp.where(odd, near_east, near_west)


def open_kernel(
    core_ref,
    odd_ref,
    mine_ref,
    other_ref,
    zero_ref,
    above_ref,
    one_ref,
    two_ref,
    decay_ref,
    power_ref,
    turn_ref,
    terms_ref,
    weigh_ref,
    carry_ref,
):
    low = core_ref[0] == 0
    lane = iota(1)
    pair = lane // 8
    even = (pair & 1) == 0

    def turned(half_ref, s):
        turn_ref[pl.ds(0, 64, stride=2), :] = jnp.where(low, half_ref[0], half_ref[1])
        turn_ref[pl.ds(1, 64, stride=2), :] = jnp.where(low, half_ref[1], half_ref[0])
        return turn_ref[...].T

    for s in range(4):
        early, late = (
            [ref[pl.ds(at + s, 64, stride=4), :] for ref in (mine_ref, other_ref)]
            for at in (0, 256)
        )
        here = turned([jnp.where(low, a, b) for a, b in zip(early, late)], s)
        behind = turned(late, s)
        for half in range(2):
            at = 64 * half
            col = s + 4 * half
            mixed = here[at + 48 : at + 56, :]
            decays = (
                jnp.where(even, mixed, pltpu.roll(mixed, 8, 1)),
                here[at + 56 : at + 64, :],
                jnp.where(even, pltpu.roll(mixed, 120, 1), mixed),
            )
            for f in range(FIELDS):
                decay = decays[f]
                decay_ref[f, col] = decay
                for j in range(2):
                    to = at + 24 * j + 8 * f
                    terms_ref[0, j, f, col] = here[to : to + 8, :]
                    terms_ref[1, j, f, col] = behind[to : to + 8, :]
                square = decay * decay
                power_ref[0, f, col] = powers(square, 16 - pair)
                power_ref[1, f, col] = decay * powers(square, 15 - pair, (1, 2, 4, 8))
    chain_first(
        lambda f, col: (terms_ref[1, 0, f, col], terms_ref[1, 1, f, col]),
        decay_ref,
        None,
        carry_ref,
        weigh_ref,
    )
    for f in range(FIELDS):
        for col in range(LONS):
            decay = decay_ref[f, col]
            c0, c1 = terms_ref[0, 0, f, col], terms_ref[0, 1, f, col]
            carry = jnp.where(low, carry_ref[f, col], 0.0)
            c1 = c1 + jnp.where(pair == 15, decay * carry, 0.0)
            value, second = chain_local(c0 + decay * c1, c1, decay, pair)
            zero_ref[f, col] = value
            above_ref[0, f, col] = second
            above_ref[1, f, col] = jnp.where(pair < 15, later(value, 1), carry)
    send_halo(odd_ref, above_ref, one_ref, two_ref)


def close_kernel(
    core_ref,
    odd_ref,
    first_ref,
    second_ref,
    carry_ref,
    power_ref,
    zero_ref,
    above_ref,
    one_ref,
    two_ref,
):
    low = core_ref[0] == 0
    pair = iota(1) // 8
    for f in range(FIELDS):
        for col in range(LONS):
            carry = jnp.where(low, carry_ref[f, col], 0.0)
            value = first_ref[f, col] + power_ref[0, f, col] * carry
            zero_ref[f, col] = value
            above_ref[0, f, col] = second_ref[f, col] + power_ref[1, f, col] * carry
            above_ref[1, f, col] = jnp.where(pair < 15, later(value, 1), carry)
    send_halo(odd_ref, above_ref, one_ref, two_ref)


def fine_kernel(
    odd_ref, own_ref, one_ref, two_ref, decay_ref, pairs_ref, *rest
):
    carry_ref, state_ref, weigh_ref = rest if len(rest) == 3 else (None, *rest, None)
    odd = odd_ref[0] == 1
    lane = iota(1)
    band = lane % 8
    width = 3 * LONS

    def slot(j, f, col):
        return 24 * ((j * FIELDS + f) * width + col)

    def put(j, f, col, value):
        at = slot(j, f, col) + 8
        state_ref[at : at + 8, :] = value

    def here(j, f, col):
        at = slot(j, f, col) + 8
        return state_ref[at : at + 8, :]

    def rows(j, f, col):
        at = slot(j, f, col) + 8
        return state_ref[at + 1 : at + 9, :], state_ref[at - 1 : at + 7, :]

    def edges(j, f, low, high):
        for col in range(low, high, 8):
            at = slot(j, f, min(col, width - 8))
            first = pltpu.roll(state_ref[pl.ds(at + 8, 8, stride=24), :], 127, 1)
            last = pltpu.roll(state_ref[pl.ds(at + 15, 8, stride=24), :], 1, 1)
            state_ref[pl.ds(at + 16, 8, stride=24), :] = jnp.where(band < 7, first, 0.0)
            state_ref[pl.ds(at + 7, 8, stride=24), :] = jnp.where(band > 0, last, 0.0)

    for j in range(2):
        for f in range(FIELDS):
            skipped = 1 if f == 2 else 0
            for at in range(LONS - skipped):
                one, two = one_ref[j, LONS * f + at], two_ref[j, LONS * f + at]
                put(j, f, at + skipped, jnp.where(odd, one, two))
                put(j, f, 2 * LONS + at, jnp.where(odd, two, one))
            for at in range(LONS):
                put(j, f, LONS + at, own_ref[j, f, at])
            if skipped:
                put(j, f, 0, jnp.zeros((8, 128), jnp.float32))
                put(j, f, width - 1, jnp.zeros((8, 128), jnp.float32))
            edges(j, f, 0, width)

    keep = 1.0 / diffusion - 4.0
    wave = 0.5 * wave_coef / diffusion
    wave_new = 0.5 * wave_coef
    turn = coriolis / diffusion
    unit = diffusion**STEPS
    result = {}
    for step in range(STEPS):
        low, high = 2 * step + 1, width - 2 * step - 1
        for j in range(2):
            p = {col: here(j, 0, col) for col in (low - 1, low)}
            q = {col: here(j, 1, col) for col in (low - 1, low)}
            for col in range(low, high):
                p[col + 1], q[col + 1] = here(j, 0, col + 1), here(j, 1, col + 1)
                p_next, p_last = rows(j, 0, col)
                r_next, r_last = rows(j, 2, col)
                p1 = ((keep * p[col] + (p[col - 1] + p[col + 1])) + (p_next + p_last)) + wave * (
                    (q[col + 1] - q[col - 1]) + (r_next - r_last)
                )
                put(j, 0, col, p1)
            edges(j, 0, low, high)
        low, high = low + 1, high - 1
        for j in range(2):
            p, q, r = (
                {col: here(j, f, col) for col in (low - 1, low)} for f in range(FIELDS)
            )
            for col in range(low, high):
                p[col + 1], q[col + 1], r[col + 1] = (here(j, f, col + 1) for f in range(FIELDS))
                p_next, p_last = rows(j, 0, col)
                q_next, q_last = rows(j, 1, col)
                r_next, r_last = rows(j, 2, col)
                q1 = (
                    (keep * q[col] + (q[col - 1] + q[col + 1])) + (q_next + q_last)
                ) + (wave_new * (p[col + 1] - p[col - 1]) + turn * r[col])
                r1 = (
                    (keep * r[col] + (r[col - 1] + r[col + 1])) + (r_next + r_last)
                ) + (wave_new * (p_next - p_last) - turn * q[col])
                if step < STEPS - 1:
                    put(j, 1, col, q1)
                    if low < col < high - 1:
                        put(j, 2, col, r1)
                else:
                    for f, value in enumerate((p[col], q1, r1)):
                        result[j, f, col - LONS] = value
            if step < STEPS - 1:
                edges(j, 1, low, high)
                edges(j, 2, low, high)

    def terms(f, col):
        return [unit * result[j, f, col] - decay_ref[f, col] * own_ref[j, f, col] for j in range(2)]

    chain_first(terms, decay_ref, pairs_ref, carry_ref, weigh_ref)


def emphases(core):
    first = (2 * (iota(1) // 8 + 16 * core)).astype(jnp.float32)
    return [1.0 + 2.0 * (first + j) / 63.0 for j in range(2)]


def so_far_kernel(core_ref, *refs):
    zeros, aboves = refs[0:ITERS], refs[ITERS : 2 * ITERS]
    misfit_ref, out_ref = refs[2 * ITERS :]
    emphasis = emphases(core_ref[0])
    sums = [jnp.zeros((8, 128), jnp.float32) for _ in range(2 * ITERS - 2)]
    for f in range(FIELDS):
        for col in range(LONS):
            for j in range(2):
                parts = [
                    zeros[n][f, col] if j == 0 else aboves[n][0, f, col] for n in range(ITERS)
                ]
                total = parts[0]
                for n in range(1, ITERS):
                    total = total + parts[n]
                    changed, size = emphasis[j] * (parts[n] * parts[n]), emphasis[j] * (total * total)
                    sums[n - 1] = sums[n - 1] + changed
                    sums[ITERS + n - 2] = sums[ITERS + n - 2] + size
                out_ref[(j * FIELDS + f) * LONS + col] = total
    for at, value in enumerate(sums + [misfit_ref[...]]):
        out_ref[CELLS + at] = value


def finish_kernel(
    core_ref,
    first_ref,
    second_ref,
    pairs_ref,
    other_pairs_ref,
    total_ref,
    other_total_ref,
    decay_ref,
    power_ref,
    out_ref,
    weigh_ref,
    carry_ref,
    turn_ref,
    back_ref,
):
    low = core_ref[0] == 0
    pair = iota(1) // 8
    chain_first(
        lambda f, col: None,
        decay_ref,
        None,
        carry_ref,
        weigh_ref,
        both_of=lambda f, col: jnp.where(low, other_pairs_ref[0, f, col], pairs_ref[0, f, col]),
    )
    change = size = jnp.zeros((8, 128), jnp.float32)
    result = {}
    emphasis = emphases(core_ref[0]), emphases(1 - core_ref[0])
    for f in range(FIELDS):
        for col in range(LONS):
            decay, carry = decay_ref[f, col], carry_ref[f, col]
            mine, others = jnp.where(low, carry, 0.0), jnp.where(low, 0.0, carry)
            enters = jnp.where(pair == 15, decay * others, 0.0)
            values = (
                (
                    first_ref[f, col] + power_ref[0, f, col] * mine,
                    second_ref[f, col] + power_ref[1, f, col] * mine,
                ),
                chain_local(
                    other_pairs_ref[0, f, col] + decay * enters,
                    other_pairs_ref[1, f, col] + enters,
                    decay,
                    pair,
                ),
            )
            for side, ref in enumerate((total_ref, other_total_ref)):
                for j in range(2):
                    value = values[side][j]
                    total = ref[(j * FIELDS + f) * LONS + col] + value
                    change = change + emphasis[side][j] * (value * value)
                    size = size + emphasis[side][j] * (total * total)
                    result[side, j, f, col] = total
    row = iota(0)
    sums = [total_ref[CELLS + at] + other_total_ref[CELLS + at] for at in range(2 * ITERS - 1)]
    counted = sums[0 : ITERS - 1] + [change, sums[-1]] + sums[ITERS - 1 : 2 * ITERS - 2] + [size]
    parts = jnp.zeros((8, 128), jnp.float32)
    for at, part in enumerate(counted):
        parts = jnp.where(row == at, jnp.sum(part, axis=0, keepdims=True), parts)
    ones = jnp.ones((128, 128), jnp.float32)
    turn_ref[48:56, :] = jnp.dot(parts, ones, precision=lax.Precision.HIGHEST)
    for s in range(4):
        kept = []
        for which in range(2):
            for side in range(2):
                for j in range(2):
                    for f in range(FIELDS):
                        to = 64 * side + 24 * j + 8 * f
                        turn_ref[to : to + 8, :] = result[which, j, f, s + 4 * side]
            back_ref[...] = turn_ref[...].T
            evens = back_ref[pl.ds(0, 64, stride=2), :]
            odds = back_ref[pl.ds(1, 64, stride=2), :]
            kept.append(jnp.where(low, evens, odds))
        out_ref[pl.ds(s, 64, stride=4), :] = jnp.where(low, kept[0], kept[1])
        out_ref[pl.ds(256 + s, 64, stride=4), :] = jnp.where(low, kept[1], kept[0])


def unpack_kernel(in_ref, out_ref, misfit_ref, changes_ref, rows_ref):
    sums = [in_ref[pl.ds(32 * v, 8, stride=4), :] for v in range(16)]
    while len(sums) > 1:
        sums = [a + b for a, b in zip(sums[::2], sums[1::2])]
    total = pltpu.roll(jnp.broadcast_to(jnp.sum(sums[0], axis=0, keepdims=True), (8, 128)), 80, 1)
    misfit_ref[...] = total[0:1, 3:4]
    changes_ref[...] = (total / (pltpu.roll(total, 124, 1) + epsilon))[0:1, 0:ITERS]
    second = (lax.broadcasted_iota(jnp.int32, (128, 128), 0) & 7) >= 4
    for b in range(8):
        for i in range(16):
            at = 4 * chip_of(16 * b + i)
            piece = in_ref[at : at + 4, :]
            rows_ref[8 * i : 8 * i + 4, :] = piece
            rows_ref[8 * i + 4 : 8 * i + 8, :] = piece
        block = rows_ref[...]
        turned = jnp.where(second, pltpu.roll(block, 64, 1), block).T
        for j in range(2):
            for f in range(FIELDS):
                at = 24 * j + 8 * f
                out_ref[j, f, :, 128 * b : 128 * b + 128] = turned[at : at + 8, :]


def per_device(departure, obs_weight, obs_block, coarse_decay):
    z, y, x, core = (lax.axis_index(name) for name in ("z", "y", "x", "c"))
    core_arg = core.astype(jnp.int32).reshape(1)
    tile_odd = ((x + y + z + core) % 2).astype(jnp.int32).reshape(1)
    place = (z * NY + y).astype(jnp.int32).reshape(1)

    position = ((z * NY + y) * 2 + jnp.arange(2)).astype(jnp.float32)
    strength = (1.0 + 2.0 * position / 63.0)[:, None] * obs_weight
    misfit_part = 0.5 * jnp.sum(
        strength[:, :, None, None] * departure * departure, axis=(0, 1, 2)
    ).reshape(8, 128)

    sent = call(
        pack_kernel,
        shape(512, 128),
        (place,),
        far=(departure.transpose(0, 2, 1, 3), obs_weight, obs_block, coarse_decay),
        scratch=[
            pltpu.VMEM((2, FIELDS, 16, 1024), jnp.float32),
            pltpu.VMEM((2, 16), jnp.float32),
            pltpu.VMEM((2, 16), jnp.int32),
            pltpu.VMEM((FIELDS, 8, 1024), jnp.float32),
            pltpu.VMEM((512, 128), jnp.float32),
            pltpu.SemaphoreType.DMA((4,)),
        ],
    )
    got = lax.all_to_all(sent.reshape(CHIPS, 4, 128), ZYX, 0, 0).reshape(512, 128)
    other = lax.ppermute(got, "c", SIBLING)

    field = shape(FIELDS, LONS, 8, 128)
    both = shape(2, FIELDS, LONS, 8, 128)
    square = pltpu.VMEM((128, 128), jnp.float32)
    weigh = pltpu.VMEM((FIELDS * LONS * 8, 128), jnp.float32)
    halo = shape(2, LONS * FIELDS - 1, 8, 128)
    zero, above, to_one, to_two, decay, power = call(
        open_kernel,
        (field, both, halo, halo, field, both),
        (core_arg, tile_odd),
        got,
        other,
        scratch=[
            square,
            pltpu.VMEM((2, 2, FIELDS, LONS, 8, 128), jnp.float32),
            weigh,
            pltpu.VMEM((FIELDS, LONS, 8, 128), jnp.float32),
        ],
    )
    zeros, aboves = [], []
    for iteration in range(ITERS):
        if iteration > 0:
            zero, above, to_one, to_two = call(
                close_kernel,
                (field, both, halo, halo),
                (core_arg, tile_odd),
                first,
                second,
                carry,
                power,
            )
        zeros.append(zero)
        aboves.append(above)
        side_one = lax.ppermute(to_one, ALL, swap_pairs(0))
        side_two = lax.ppermute(to_two, ALL, swap_pairs(1))
        last = iteration == ITERS - 1
        found = call(
            fine_kernel,
            both if last else (both, field),
            (tile_odd,),
            above,
            side_one,
            side_two,
            decay,
            scratch=[pltpu.VMEM((2 * FIELDS * 3 * LONS * 24, 128), jnp.float32)]
            + ([] if last else [weigh]),
        )
        pairs, carry = (found, None) if last else found
        if not last:
            carry = lax.ppermute(carry, "c", SIBLING)
        first, second = call(scan_kernel, (field, field), (), pairs, decay)
    total = call(
        so_far_kernel,
        shape(CELLS + 2 * ITERS - 1, 8, 128),
        (core_arg,),
        *zeros,
        *aboves,
        misfit_part,
    )
    other_total, other_pairs = (lax.ppermute(value, "c", SIBLING) for value in (total, pairs))
    back = call(
        finish_kernel,
        shape(512, 128),
        (core_arg,),
        first,
        second,
        pairs,
        other_pairs,
        total,
        other_total,
        decay,
        power,
        scratch=[weigh, pltpu.VMEM((FIELDS, LONS, 8, 128), jnp.float32), square, square],
    )
    home = lax.all_to_all(back.reshape(CHIPS, 4, 128), ZYX, 0, 0).reshape(512, 128)
    adjoint, misfit, changes = call(
        unpack_kernel,
        (
            jax.ShapeDtypeStruct((2, FIELDS, 8, 1024), jnp.float32),
            jax.ShapeDtypeStruct((1, 1), jnp.float32),
            jax.ShapeDtypeStruct((1, ITERS), jnp.float32),
        ),
        (),
        home,
        scratch=[square],
    )
    return adjoint, misfit.reshape(()), changes.reshape(ITERS)


def solution(mesh):
    split = Mesh(mesh.devices.reshape(NZ, NY, NX, 2), ("z", "y", "x", "c"))
    return jax.shard_map(
        per_device,
        mesh=split,
        in_specs=(P(TM, GRID, None, None), P(TM, GRID), P(TM, GRID), P(None, GRID, None)),
        out_specs=(P(TM, None, GRID, None), P(), P()),
        check_vma=False,
    )
```
